32 devices in a mesh: seq: 8 (over z, y), head: 4 (over x, core).
Axes of the slice: x: 2, y: 2, z: 4, core: 2. Of those that a mesh axis runs over, the one named last changes fastest.
Arguments:
- tokens: bfloat16 [8192, 1536], P('seq', 'head'), may hold values from -6 to 6
- segment_ids: int32 [8192], replicated, may hold values from 0 to 7, never falling along the last dimension, each value on 1 to 2000 neighbouring positions
- first_gain: float32 [1536], P('head'), may hold values from 0.5 to 1.5
- proj_zx: bfloat16 [1536, 2, 3072], P(None, None, 'head'), may hold values from -0.15625 to 0.15625
- proj_bc: bfloat16 [1536, 256], replicated, may hold values from -0.15625 to 0.15625
- proj_step: bfloat16 [1536, 48], P(None, 'head'), may hold values from -0.3125 to 0.3125
- conv_inner: float32 [4, 3072], P(None, 'head'), may hold values from -3 to 3
- conv_inner_bias: float32 [3072], P('head'), may hold values from -1.8 to 1.8
- conv_state: float32 [4, 256], replicated, may hold values from -3 to 3
- conv_state_bias: float32 [256], replicated, may hold values from -1.8 to 1.8
- step_bias: float32 [48], P('head'), may hold values from -5 to 0
- decay_log: float32 [48], P('head'), may hold values from -8 to 1
- skip_scale: float32 [48], P('head'), may hold values from 0.5 to 1.5
- gated_gain: float32 [3072], P('head'), may hold values from 0.5 to 1.5
- proj_out: bfloat16 [3072, 1536], P('head'), may hold values from -0.109375 to 0.109375
- second_gain: float32 [1536], P('head'), may hold values from 0.5 to 1.5
- proj_qkv: bfloat16 [1536, 3, 1536], P(None, None, 'head'), may hold values from -0.15625 to 0.15625
- attention_out: bfloat16 [1536, 1536], P('head'), may hold values from -0.625 to 0.625
- cotangent: bfloat16 [8192, 1536], P('seq', 'head'), may hold values from -6 to 6
Outputs:
- output: bfloat16 [8192, 1536], P('seq', 'head')
- grad_tokens: bfloat16 [8192, 1536], P('seq', 'head')
- grad_first_gain: float32 [1536], P('head')
- grad_proj_zx: float32 [1536, 2, 3072], P('seq', None, 'head')
- grad_proj_bc: float32 [1536, 256], P(None, ('seq', 'head'))
- grad_proj_step: float32 [1536, 48], P('seq', 'head')
- grad_conv_inner: float32 [4, 3072], P(None, 'head')
- grad_conv_inner_bias: float32 [3072], P('head')
- grad_conv_state: float32 [4, 256], P(None, ('seq', 'head'))
- grad_conv_state_bias: float32 [256], P(('seq', 'head'))
- grad_step_bias: float32 [48], P('head')
- grad_decay_log: float32 [48], P('head')
- grad_skip_scale: float32 [48], P('head')
- grad_gated_gain: float32 [3072], P('head')
- grad_proj_out: float32 [3072, 1536], P('head', 'seq')
- grad_second_gain: float32 [1536], P('head')
- grad_proj_qkv: float32 [1536, 3, 1536], P('seq', None, 'head')
- grad_attention_out: float32 [1536, 1536], P('head', 'seq')
The draws below stay inside these ranges and needn't reach their ends.
Inputs may be any that keep to these rules, and one draw needn't show every extreme that they name: `segment_ids`: ids never fall along the sequence; a document (run of equal ids) has at most 2000 tokens, and some document has exactly 2000.
All inputs are finite; a program needn't handle non-finite values.
Results may differ from the reference program's by a relative error of at most 0.03.
Values may be sent and summed in bfloat16 or wider, within the bound.
A program may use at most 448 MiB of HBM per device.

```python
import math
from functools import partial
import jax
import jax.numpy as jnp
import numpy as np
from jax import lax

D = 1536
SSM_HEADS = 48
SSM_DIM = 64
STATE = 128
ATT_HEADS = 24
ATT_DIM = 64
SPAN = 256
CONV = 4
DOC_MAX = 2000
TOK_DEV = 1024
INNER = 3072
TOKENS = 8192
REACH = 2
N_HEAD = 4


def level_of(rng, shape, cuts, low, high):
    level = 1.0
    for dim, shards_of in cuts:
        draws = jax.random.uniform(jax.random.fold_in(jax.random.fold_in(rng, 6), dim), (shards_of,), jnp.float32, low / len(cuts), high / len(cuts))
        level = level * jnp.repeat(jnp.exp(draws), shape[dim] // shards_of).reshape((-1,) + (1,) * (len(shape) - 1 - dim))
    return level


def length_profile(amount, total, reach, skew):
    portions = [(1 << 20) // math.isqrt(rank ** skew) + 1 for rank in range(2, amount + 1)]
    spare, holding = total - reach - (amount - 1), [1] * (amount - 1)
    while spare > 0:
        movable = [i for i in range(amount - 1) if holding[i] < reach]
        mass, left = sum([portions[i] for i in movable]), spare
        for i in movable:
            extra = min(reach - holding[i], max(1, left * portions[i] // mass), spare)
            holding[i] = holding[i] + extra
            spare = spare - extra
    return np.array([reach] + holding)


def ragged(key, count, total, reach, slope):
    if count == 2:
        one = jax.random.randint(key, (), max(1, total - reach), min(reach, total - 1) + 1)
        return jnp.stack([one, total - one])
    sizes = jnp.asarray(length_profile(count, total, reach, slope), jnp.int32)
    pairs = (count - 1) // 2
    donor, taker = sizes[1:1 + 2 * pairs:2], sizes[2:2 + 2 * pairs:2]
    margin = jnp.minimum(donor - 1, reach - taker)
    passed = jax.random.randint(jax.random.fold_in(key, 1), (pairs,), 0, 1 << 20) % (margin + 1)
    sizes = sizes.at[1:1 + 2 * pairs:2].set(donor - passed).at[2:2 + 2 * pairs:2].set(taker + passed)
    return sizes[jax.random.permutation(jax.random.fold_in(key, 2), count)]


def normal_values(stream_key, dims, deviation, limit, pieces=(), held_as=jnp.bfloat16):
    entries = jax.random.normal(stream_key, dims, jnp.float32) * deviation
    if len(pieces) > 0:
        entries = level_of(stream_key, dims, pieces, -0.22, 0.18) * entries
    return jnp.clip(entries, min=-limit, max=limit).astype(held_as)


def setup_inputs(seed: int = 0) -> dict:
    seeds = jax.random.split(jax.random.key(seed), 20)
    return {
        "tokens": normal_values(seeds[0], (TOKENS, D), 1.0, 6.0, ((0, 8), (1, 4))),
        "segment_ids": jnp.searchsorted(jnp.cumsum(ragged(seeds[1], TOKENS // (DOC_MAX // 2), TOKENS, DOC_MAX, 1)), jnp.arange(TOKENS), side="right").astype(jnp.int32),
        "first_gain": jnp.clip(1.0 + 0.1 * jax.random.normal(seeds[2], (D,), jnp.float32), 0.5, 1.5),
        "proj_zx": normal_values(seeds[3], (D, 2, INNER), D ** -0.5, 0.15625, ((2, 4),)),
        "proj_bc": normal_values(seeds[4], (D, 2 * STATE), D ** -0.5, 0.15625),
        "proj_step": normal_values(seeds[5], (D, SSM_HEADS), (D // 4) ** -0.5, 0.3125, ((1, 4),)),
        "conv_inner": normal_values(seeds[6], (CONV, INNER), CONV ** -0.5, 3.0, ((1, 4),), jnp.float32),
        "conv_inner_bias": normal_values(seeds[7], (INNER,), 0.3, 1.8, ((0, 4),), jnp.float32),
        "conv_state": normal_values(seeds[8], (CONV, 2 * STATE), CONV ** -0.5, 3.0, (), jnp.float32),
        "conv_state_bias": normal_values(seeds[9], (2 * STATE,), 0.3, 1.8, (), jnp.float32),
        "step_bias": jnp.clip(-5.0 + 5.0 * jax.random.uniform(seeds[10], (SSM_HEADS,), jnp.float32) ** level_of(seeds[10], (SSM_HEADS,), ((0, 4),), -0.2, 0.2), -5.0, 0.0),
        "decay_log": jnp.clip(-8.0 + 9.0 * jax.random.uniform(seeds[11], (SSM_HEADS,), jnp.float32) ** level_of(seeds[11], (SSM_HEADS,), ((0, 4),), -0.2, 0.2), -8.0, 1.0),
        "skip_scale": jnp.clip(0.5 + 1.0 * jax.random.uniform(seeds[12], (SSM_HEADS,), jnp.float32) ** level_of(seeds[12], (SSM_HEADS,), ((0, 4),), -0.2, 0.2), 0.5, 1.5),
        "gated_gain": jnp.clip(1.0 + 0.1 * jax.random.normal(seeds[13], (INNER,), jnp.float32), 0.5, 1.5),
        "proj_out": normal_values(seeds[14], (INNER, D), INNER ** -0.5, 0.109375, ((0, 4),)),
        "second_gain": jnp.clip(1.0 + 0.1 * jax.random.normal(seeds[15], (D,), jnp.float32), 0.5, 1.5),
        "proj_qkv": normal_values(seeds[16], (D, 3, ATT_HEADS * ATT_DIM), D ** -0.5, 0.15625, ((2, 4),)),
        "attention_out": normal_values(seeds[17], (ATT_HEADS * ATT_DIM, D), (ATT_HEADS * ATT_DIM // 16) ** -0.5, 0.625, ((0, 4),)),
        "cotangent": normal_values(seeds[18], (TOKENS, D), 1.0, 6.0, ((0, 8), (1, 4))),
    }


epsilon = 1e-05
highest = lax.Precision.HIGHEST
masked_score = -1e+30

@jax.custom_vjp
def low(v):
    return lax.optimization_barrier(v.astype(jnp.bfloat16)).astype(jnp.float32)

@jax.custom_vjp
def low_back(v):
    return v

def low_keep(v):
    return (low(v), None)

def low_pass(kept, grad):
    return (grad,)

def back_keep(v):
    return (v, None)

def back_low(kept, grad):
    return (low(grad),)
low.defvjp(low_keep, low_pass)
low_back.defvjp(back_keep, back_low)

def exact_dot(left, right):
    return jnp.dot(left, right, precision=highest, preferred_element_type=jnp.float32)

def row_norm(hidden, gain):
    return hidden * lax.rsqrt(lax.optimization_barrier(jnp.mean(hidden * hidden, axis=-1, keepdims=True)) + epsilon) * gain

def conv_piece(conv_input, edge_rows, conv_weight, conv_bias, local_seg, edge_seg):
    row_count = conv_input.shape[0]
    padded = jnp.concatenate([edge_rows, conv_input], axis=0)
    padded_seg = jnp.concatenate([edge_seg, local_seg])
    summed = jnp.zeros(conv_input.shape, jnp.float32) + conv_bias[None, :]
    for tap_index in range(conv_weight.shape[0]):
        kept = (padded_seg[tap_index:tap_index + row_count] == local_seg).astype(jnp.float32)
        summed = summed + conv_weight[tap_index][None, :] * padded[tap_index:tap_index + row_count] * kept[:, None]
    return jax.nn.silu(summed)

def causal_conv(conv_input, segment_ids, conv_weight, conv_bias):
    edge_rows = jnp.zeros((CONV - 1, conv_input.shape[1]), jnp.float32)
    edge_seg = jnp.full((CONV - 1,), -1, jnp.int32)
    return conv_piece(conv_input, edge_rows, conv_weight, conv_bias, segment_ids, edge_seg)

def ssd_span(ssd_state, span_data):
    values, state_b, state_c, step_sizes, decay_rates, seg_block, prev_seg = span_data
    length = seg_block.shape[0]
    cumulative = jnp.cumsum(decay_rates, axis=0)
    causal = jnp.arange(length)[:, None] >= jnp.arange(length)[None, :]
    allowed = ((seg_block[:, None] == seg_block[None, :]) & causal).astype(jnp.float32)[:, :, None]
    spread = cumulative[:, None, :] - cumulative[None, :, :]
    decay_pairs = jnp.exp(jnp.where(allowed > 0, spread, 0.0)) * allowed
    intersection = jnp.dot(state_c, state_b.T, precision=highest, preferred_element_type=jnp.float32)
    mixing = intersection[:, :, None] * decay_pairs * step_sizes[None, :, :]
    within = jnp.einsum('tsh,shp->thp', mixing, values, precision=highest)
    entering = jnp.exp(cumulative) * (seg_block == prev_seg).astype(jnp.float32)[:, None]
    carried = jnp.einsum('tn,hpn->thp', state_c, ssd_state, precision=highest) * entering[:, :, None]
    last_seg = seg_block[length - 1]
    tail_weight = jnp.exp(cumulative[length - 1][None, :] - cumulative) * (seg_block == last_seg).astype(jnp.float32)[:, None] * step_sizes
    fresh = jnp.einsum('shp,sn->hpn', tail_weight[:, :, None] * values, state_b, precision=highest)
    through = jnp.exp(cumulative[length - 1]) * (last_seg == prev_seg).astype(jnp.float32)
    return (ssd_state * through[:, None, None] + fresh, within + carried)

def ssd_sequence(inner_u, state_bc, step_raw, step_bias, decay_log, skip_scale, segment_ids):
    row_count, head_count = step_raw.shape
    head_size = inner_u.shape[1] // head_count
    state_width = state_bc.shape[1] // 2
    blocks = row_count // SPAN
    values = inner_u.reshape(row_count, head_count, head_size)
    step_sizes = jax.nn.softplus(step_raw + step_bias)
    decay_rates = -jnp.exp(decay_log) * step_sizes
    prev_all = jnp.concatenate([jnp.full((1,), -1, jnp.int32), segment_ids[:-1]])
    span_prev = prev_all.reshape(blocks, SPAN)[:, 0]
    start_state = jnp.zeros((head_count, head_size, state_width), jnp.float32)
    inputs = (values.reshape(blocks, SPAN, head_count, head_size), state_bc[:, :state_width].reshape(blocks, SPAN, state_width), state_bc[:, state_width:].reshape(blocks, SPAN, state_width), step_sizes.reshape(blocks, SPAN, head_count), decay_rates.reshape(blocks, SPAN, head_count), segment_ids.reshape(blocks, SPAN), span_prev)
    end_state, outputs = lax.scan(jax.checkpoint(ssd_span), start_state, inputs)
    outputs = outputs.reshape(row_count, head_count, head_size) + skip_scale[None, :, None] * values
    return outputs.reshape(row_count, head_count * head_size)

def attend_block(query_block, key_window, value_window, query_seg, key_seg, query_pos, key_pos):
    score_scale = 1.0 / math.sqrt(query_block.shape[2])
    scores = low_back(jnp.einsum('qhd,khd->hqk', query_block, key_window, precision=highest) * score_scale)
    allowed = (query_seg[:, None] == key_seg[None, :]) & (key_pos[None, :] <= query_pos[:, None])
    scores = jnp.where(allowed[None], scores, masked_score)
    row_top = lax.optimization_barrier(jnp.max(scores, axis=2, keepdims=True))
    exp_scores = jnp.exp(scores - row_top)
    weights = exp_scores / lax.optimization_barrier(jnp.sum(exp_scores, axis=2, keepdims=True))
    return jnp.einsum('hqk,khd->qhd', low(weights), value_window, precision=highest)

def attention(queries, keys, values, segment_ids):
    total_rows = queries.shape[0]
    front = REACH * TOK_DEV
    key_pad = jnp.concatenate([jnp.zeros((front,) + keys.shape[1:], jnp.float32), keys], axis=0)
    value_pad = jnp.concatenate([jnp.zeros((front,) + values.shape[1:], jnp.float32), values], axis=0)
    seg_pad = jnp.concatenate([jnp.full((front,), -1, jnp.int32), segment_ids])
    pos_pad = jnp.arange(total_rows + front, dtype=jnp.int32) - front
    query_pos_all = jnp.arange(total_rows, dtype=jnp.int32)

    def one_block(start):
        query_block = lax.dynamic_slice_in_dim(queries, start, TOK_DEV)
        key_window = lax.dynamic_slice_in_dim(key_pad, start, front + TOK_DEV)
        value_window = lax.dynamic_slice_in_dim(value_pad, start, front + TOK_DEV)
        query_seg = lax.dynamic_slice_in_dim(segment_ids, start, TOK_DEV)
        key_seg = lax.dynamic_slice_in_dim(seg_pad, start, front + TOK_DEV)
        query_pos = lax.dynamic_slice_in_dim(query_pos_all, start, TOK_DEV)
        key_pos = lax.dynamic_slice_in_dim(pos_pad, start, front + TOK_DEV)
        return attend_block(query_block, key_window, value_window, query_seg, key_seg, query_pos, key_pos)
    starts = (jnp.arange(total_rows // TOK_DEV) * TOK_DEV).astype(jnp.int32)
    blocks_out = lax.map(jax.checkpoint(one_block), starts)
    return blocks_out.reshape(queries.shape)

def forward(segment_ids, hidden_zero, first_gain, proj_zx, proj_bc, proj_step, conv_inner, conv_inner_bias, conv_state, conv_state_bias, step_bias, decay_log, skip_scale, gated_gain, proj_out, second_gain, proj_qkv, attention_out):
    row_count = hidden_zero.shape[0]
    first_norm = low(row_norm(hidden_zero, first_gain))
    zx_proj = low_back(exact_dot(first_norm, proj_zx.reshape(D, 2 * INNER)))
    gate_z = zx_proj[:, :INNER]
    inner_x = zx_proj[:, INNER:]
    bc_proj = exact_dot(first_norm, proj_bc)
    step_raw = low_back(exact_dot(first_norm, proj_step))
    inner_u = causal_conv(inner_x, segment_ids, conv_inner, conv_inner_bias)
    group_heads = SSM_HEADS // N_HEAD
    group_width = group_heads * SSM_DIM
    group_outputs = []
    for group_index in range(N_HEAD):
        state_bc = causal_conv(low_back(bc_proj), segment_ids, conv_state, conv_state_bias)
        first_head = group_index * group_heads
        first_channel = group_index * group_width
        group_outputs.append(ssd_sequence(inner_u[:, first_channel:first_channel + group_width], state_bc, step_raw[:, first_head:first_head + group_heads], step_bias[first_head:first_head + group_heads], decay_log[first_head:first_head + group_heads], skip_scale[first_head:first_head + group_heads], segment_ids))
    ssd_out = jnp.concatenate(group_outputs, axis=1)
    mixed = ssd_out * jax.nn.silu(gate_z)
    gated = low(row_norm(mixed, gated_gain))
    hidden_one = hidden_zero + low_back(exact_dot(gated, proj_out))
    second_norm = low(row_norm(hidden_one, second_gain))
    att_width = ATT_HEADS * ATT_DIM
    projected = low(low_back(exact_dot(second_norm, proj_qkv.reshape(D, 3 * att_width))))
    queries = projected[:, :att_width].reshape(row_count, ATT_HEADS, ATT_DIM)
    keys = projected[:, att_width:2 * att_width].reshape(row_count, ATT_HEADS, ATT_DIM)
    values = projected[:, 2 * att_width:].reshape(row_count, ATT_HEADS, ATT_DIM)
    attended = attention(queries, keys, values, segment_ids)
    attended = low(low_back(attended.reshape(row_count, att_width)))
    return hidden_one + low_back(exact_dot(attended, attention_out))

def reference(tokens, segment_ids, first_gain, proj_zx, proj_bc, proj_step, conv_inner, conv_inner_bias, conv_state, conv_state_bias, step_bias, decay_log, skip_scale, gated_gain, proj_out, second_gain, proj_qkv, attention_out, cotangent):
    params = [item.astype(jnp.float32) for item in (tokens, first_gain, proj_zx, proj_bc, proj_step, conv_inner, conv_inner_bias, conv_state, conv_state_bias, step_bias, decay_log, skip_scale, gated_gain, proj_out, second_gain, proj_qkv, attention_out)]
    output, pullback = jax.vjp(partial(forward, segment_ids), *params)
    grads = pullback(cotangent.astype(jnp.float32))
    return (output.astype(jnp.bfloat16), grads[0].astype(jnp.bfloat16), grads[1], grads[2], grads[3], grads[4], grads[5], grads[6], grads[7], grads[8], grads[9], grads[10], grads[11], grads[12], grads[13], grads[14], grads[15], grads[16])
```

```python
from functools import partial
import math

import jax
import jax.numpy as jnp
from jax import lax
from jax.experimental import pallas as pl
from jax.experimental.pallas import tpu as pltpu
from jax.sharding import PartitionSpec as P

D = 1536
ATT_DIM = 64
SSM_DIM = 64
SPAN = 256
CONV = 4
DOC_MAX = 2000
INNER = 3072
LANES = 128

epsilon = 1e-05
highest = lax.Precision.HIGHEST
f32 = jnp.float32
bf16 = jnp.bfloat16
masked_score = -1e30
VMEM_LIMIT = 60 * 1024 * 1024


def dot_nn(a, b, precision=None):
    return lax.dot_general(a, b, (((1,), (0,)), ((), ())), precision=precision, preferred_element_type=f32)


def dot_nt(a, b, precision=None):
    return lax.dot_general(a, b, (((1,), (1,)), ((), ())), precision=precision, preferred_element_type=f32)


def dot_tn(a, b, precision=None):
    return lax.dot_general(a, b, (((0,), (0,)), ((), ())), precision=precision, preferred_element_type=f32)


def softplus(x):
    return jnp.maximum(x, 0.0) + jnp.log1p(jnp.exp(-jnp.abs(x)))


def sigmoid(x):
    return 1.0 / (1.0 + jnp.exp(-x))


def lane_low(rows):
    return lax.broadcasted_iota(jnp.int32, (rows, LANES), 1) < SSM_DIM


def conv_rows(buf, weight, bias, kept, rows):
    summed = bias + weight[3:4, :] * buf[8 : 8 + rows, :]
    for tap in range(3):
        summed = summed + weight[tap : tap + 1, :] * (buf[5 + tap : 5 + tap + rows, :] * kept[:, tap : tap + 1])
    return summed


def fill_conv(buf, chunk, x_ref, xprev_ref, bcs_ref, bprev_ref, edge_ref, inner, rows):
    buf[8 : 8 + rows, :inner] = x_ref[...]
    buf[8 : 8 + rows, inner:] = bcs_ref[:, : buf.shape[1] - inner]

    @pl.when(chunk == 0)
    def _():
        buf[0:8, :] = edge_ref[...]

    @pl.when(chunk > 0)
    def _():
        buf[0:8, :inner] = xprev_ref[...]
        buf[0:8, inner:] = bprev_ref[:, : buf.shape[1] - inner]


def span_terms(bcs_ref, bc_width, bias_ref, rate_ref, segc_ref, segr_ref, prev, last, rows):
    raw = bcs_ref[:, bc_width:] + bias_ref[...]
    step = softplus(raw)
    decay = rate_ref[...] * step
    row = lax.broadcasted_iota(jnp.int32, (rows, rows), 0)
    col = lax.broadcasted_iota(jnp.int32, (rows, rows), 1)
    causal = row >= col
    tri = causal.astype(f32)
    cum = dot_nn(tri, decay, highest)
    segc = segc_ref[...]
    allowed = (segc == segr_ref[...]) & causal
    opened = (segc == prev).astype(f32)
    closing = (segc == last).astype(f32)
    last_cum = cum[rows - 1 : rows, :]
    enter = jnp.exp(cum) * opened
    tail = jnp.exp(last_cum - cum) * closing
    through = jnp.exp(last_cum) * (last == prev).astype(f32)
    return raw, step, decay, cum, tri, allowed, enter, tail, last_cum, through


def ssd_forward_kernel(
    prev_ref, last_ref, x_ref, xprev_ref, bcs_ref, bprev_ref, edge_ref, kept_ref, segc_ref, segr_ref,
    weight_ref, cbias_ref, bias_ref, rate_ref, skip_ref, wide_ref, tall_ref,
    y_ref, c_ref, open_ref, states_ref, end_ref, through_ref,
    state, base, buf,
):
    chunk = pl.program_id(0)
    rows = x_ref.shape[0]
    inner = x_ref.shape[1]
    width = c_ref.shape[1]
    heads = inner // SSM_DIM

    @pl.when(chunk == 0)
    def _():
        state[...] = jnp.zeros_like(state)
        base[...] = jnp.zeros_like(base)

    fill_conv(buf, chunk, x_ref, xprev_ref, bcs_ref, bprev_ref, edge_ref, inner, rows)
    pre = conv_rows(buf, weight_ref[...], cbias_ref[...], kept_ref[...], rows)
    conv = pre * sigmoid(pre)
    values = conv[:, :inner]
    b_low = conv[:, inner : inner + width].astype(bf16)
    c_low = conv[:, inner + width :].astype(bf16)
    prev, last, prev_dev = prev_ref[chunk], last_ref[chunk], prev_ref[0]
    raw, step, decay, cum, tri, allowed, enter, tail, last_cum, through = span_terms(
        bcs_ref, 2 * width, bias_ref, rate_ref, segc_ref, segr_ref, prev, last, rows
    )
    cum_t = cum.T
    inter = jnp.where(allowed, dot_nt(c_low, b_low), 0.0)
    wide = wide_ref[...]
    scaled = values * dot_nn(step, wide, highest)
    scaled_low = scaled.astype(bf16)
    old = state[...]
    old_low = old.astype(bf16)
    states_ref[...] = old_low
    c_ref[...] = c_low
    carried = dot_nt(c_low, old_low) * dot_nn(enter, wide, highest) + skip_ref[...] * values
    low = lane_low(rows)
    for pair in range(heads // 2):
        cols = slice(pair * LANES, (pair + 1) * LANES)
        both = []
        for head in (2 * pair, 2 * pair + 1):
            spread = jnp.exp(jnp.minimum(cum[:, head : head + 1] - cum_t[head : head + 1, :], 0.0))
            both.append(dot_nn((inter * spread).astype(bf16), scaled_low[:, cols]))
        y_ref[:, cols] = jnp.where(low, both[0], both[1]) + carried[:, cols]
    fresh = dot_tn((scaled * dot_nn(tail, wide, highest)).astype(bf16), b_low)
    through_rows = jnp.broadcast_to(through, (8, LANES))
    column = dot_nt(tall_ref[...], through_rows, highest)[:, 0:1]
    new = old * column + fresh
    state[...] = new
    end_ref[...] = new
    total = base[0:1, :]
    open_ref[...] = jnp.exp(total + cum) * (segc_ref[...] == prev_dev).astype(f32)
    base[...] = jnp.broadcast_to(total + last_cum, base.shape)
    through_ref[...] = jnp.broadcast_to(
        jnp.exp(total + last_cum) * (last == prev_dev).astype(f32), through_ref.shape
    )


def gate_forward_kernel(y_ref, c_ref, open_ref, enter_ref, z_ref, gain_ref, wide_ref, ssd_ref, out_ref, sum_ref):
    ssd = y_ref[...] + dot_nt(c_ref[...], enter_ref[...]) * dot_nn(open_ref[...], wide_ref[...], highest)
    z = z_ref[...]
    mixed = ssd * (z * sigmoid(z))
    ssd_ref[...] = ssd
    out_ref[...] = (mixed * gain_ref[...]).astype(bf16)
    sum_ref[...] = dot_nt(jnp.ones((8, mixed.shape[1]), f32), mixed * mixed, highest)


def gate_backward_kernel(
    bg_ref, ssd_ref, z_ref, rc_ref, gain_ref, c_ref, open_ref, wide_ref,
    dy_ref, gz_ref, gated_ref, ggain_ref, enter_ref,
):
    @pl.when(pl.program_id(0) == 0)
    def _():
        ggain_ref[...] = jnp.zeros_like(ggain_ref)
        enter_ref[...] = jnp.zeros_like(enter_ref)

    ssd = ssd_ref[...]
    z = z_ref[...]
    sig = sigmoid(z)
    gate = z * sig
    mixed = ssd * gate
    rms = rc_ref[:, 0:1]
    back = bg_ref[...].astype(f32)
    normed = mixed * rms
    gained = back * gain_ref[...]
    g_mixed = gained * rms - mixed * rc_ref[:, 1:2]
    gated_ref[...] = (normed * gain_ref[...]).astype(bf16)
    ggain_ref[...] += jnp.sum(normed * back, axis=0, keepdims=True)
    dy = (g_mixed * gate).astype(bf16)
    dy_ref[...] = dy
    gz_ref[...] = (g_mixed * ssd * (sig + gate * (1.0 - sig))).astype(bf16)
    opened = (dy.astype(f32) * dot_nn(open_ref[...], wide_ref[...], highest)).astype(bf16)
    enter_ref[...] += dot_tn(opened, c_ref[...])


def ssd_backward_kernel(
    prev_ref, last_ref, x_ref, xprev_ref, bcs_ref, bprev_ref, edge_ref, kept_ref, segc_ref, segr_ref,
    dy_ref, states_ref, openprev_ref, enter_ref, back_ref,
    weight_ref, cbias_ref, bias_ref, rate_ref, skip_ref, wide_ref, tall_ref,
    dx_ref, dbc_ref, dstep_ref, tail_ref, dedge_ref, dconv_ref, dhead_ref,
    dstate, follow, buf, grad,
):
    rows = x_ref.shape[0]
    inner = x_ref.shape[1]
    width = states_ref.shape[1]
    heads = inner // SSM_DIM
    first = pl.program_id(0) == 0
    chunk = pl.num_programs(0) - 1 - pl.program_id(0)

    @pl.when(first)
    def _():
        dstate[...] = back_ref[...]
        follow[...] = jnp.zeros_like(follow)
        dconv_ref[...] = jnp.zeros_like(dconv_ref)
        dhead_ref[...] = jnp.zeros_like(dhead_ref)

    fill_conv(buf, chunk, x_ref, xprev_ref, bcs_ref, bprev_ref, edge_ref, inner, rows)
    weight = weight_ref[...]
    kept = kept_ref[...]
    pre = conv_rows(buf, weight, cbias_ref[...], kept, rows)
    sig = sigmoid(pre)
    conv = pre * sig
    slope = sig + conv * (1.0 - sig)
    values = conv[:, :inner]
    b_low = conv[:, inner : inner + width].astype(bf16)
    c_low = conv[:, inner + width :].astype(bf16)
    prev, last = prev_ref[chunk], last_ref[chunk]
    raw, step, decay, cum, tri, allowed, enter, tail, last_cum, through = span_terms(
        bcs_ref, 2 * width, bias_ref, rate_ref, segc_ref, segr_ref, prev, last, rows
    )
    cum_t = cum.T
    inter = jnp.where(allowed, dot_nt(c_low, b_low), 0.0)
    wide = wide_ref[...]
    tall = tall_ref[...]
    step_wide = dot_nn(step, wide, highest)
    enter_wide = dot_nn(enter, wide, highest)
    tail_wide = dot_nn(tail, wide, highest)
    scaled_low = (values * step_wide).astype(bf16)
    scaled = scaled_low.astype(f32)
    dy_low = dy_ref[...]
    dy = dy_low.astype(f32)
    reach = jnp.where(chunk == 0, jnp.ones((8, LANES), f32), jnp.broadcast_to(openprev_ref[7:8, :], (8, LANES)))
    old = states_ref[...].astype(f32) + dot_nt(tall, reach, highest)[:, 0:1] * enter_ref[...].astype(f32)
    old_low = old.astype(bf16)
    dnew = dstate[...]
    dnew_low = dnew.astype(bf16)
    dy_enter = (dy * enter_wide).astype(bf16)
    from_state = dot_nt(c_low, old_low) * enter_wide
    to_state = dot_nt(b_low, dnew_low) * tail_wide
    dc = dot_nn(dy_enter, old_low)
    db = dot_nn((scaled * tail_wide).astype(bf16), dnew_low)
    through_column = dot_nt(tall, jnp.broadcast_to(through, (8, LANES)), highest)[:, 0:1]
    state_dots = jnp.sum(dnew * old, axis=1, keepdims=True) * through_column
    through_sum = jnp.sum(tall * state_dots, axis=0, keepdims=True)
    dstate[...] = dnew * through_column + dot_tn(dy_enter, c_low)
    low = lane_low(rows)
    mixed_grad = jnp.zeros((rows, rows), f32)
    within_parts = []
    dscaled_parts = []
    for pair in range(heads // 2):
        cols = slice(pair * LANES, (pair + 1) * LANES)
        scaled_pair = scaled_low[:, cols]
        dy_pair = dy_low[:, cols]
        ahead = []
        behind = []
        for index in range(2):
            head = 2 * pair + index
            spread = jnp.exp(jnp.minimum(cum[:, head : head + 1] - cum_t[head : head + 1, :], 0.0))
            mixing = (inter * spread).astype(bf16)
            dy_one = jnp.where(low if index == 0 else jnp.logical_not(low), dy_pair, jnp.zeros_like(dy_pair))
            mixed_grad = mixed_grad + dot_nt(dy_one, scaled_pair) * spread
            ahead.append(dot_nn(mixing, scaled_pair))
            behind.append(dot_tn(mixing, dy_pair))
        within_parts.append(jnp.where(low, ahead[0], ahead[1]))
        dscaled_parts.append(jnp.where(low, behind[0], behind[1]))
    within = jnp.concatenate(within_parts, axis=1)
    dscaled = jnp.concatenate(dscaled_parts, axis=1)
    mixed_low = jnp.where(allowed, mixed_grad, 0.0).astype(bf16)
    dc = dc + dot_nn(mixed_low, b_low)
    db = db + dot_tn(mixed_low, c_low)
    fresh_dots = dot_nn(scaled * to_state, tall, highest)
    dcum = dot_nn(dy * (within + from_state) - scaled * dscaled, tall, highest) - fresh_dots
    tail_sum = jnp.sum(fresh_dots, axis=0, keepdims=True) + through_sum
    ddecay = dot_tn(tri, dcum, highest) + tail_sum
    dscaled = dscaled + to_state
    dvalues = step_wide * dscaled + skip_ref[...] * dy
    dstep = dot_nn(dscaled * values, tall, highest) + ddecay * rate_ref[...]
    draw = dstep * sigmoid(raw)
    dskip = jnp.sum(dot_nn(dy * values, tall, highest), axis=0, keepdims=True)
    dhead_ref[0:1, :] += jnp.sum(draw, axis=0, keepdims=True)
    dhead_ref[1:2, :] += jnp.sum(ddecay * decay, axis=0, keepdims=True)
    dhead_ref[2:3, :] += dskip
    dstep_ref[...] = draw.astype(bf16)
    dpre = jnp.concatenate([dvalues, db, dc], axis=1) * slope
    din = weight[3:4, :] * dpre
    dconv_ref[3:4, :] += jnp.sum(dpre * buf[8 : 8 + rows, :], axis=0, keepdims=True)
    dconv_ref[4:5, :] += jnp.sum(dpre, axis=0, keepdims=True)
    dedge = jnp.zeros((8, dpre.shape[1]), f32)
    for tap in range(3):
        masked = dpre * kept[:, tap : tap + 1]
        dconv_ref[tap : tap + 1, :] += jnp.sum(masked * buf[5 + tap : 5 + tap + rows, :], axis=0, keepdims=True)
        grad[0:8, :] = jnp.zeros((8, dpre.shape[1]), f32)
        grad[8 : 8 + rows, :] = masked
        grad[8 + rows :, :] = follow[tap]
        din = din + weight[tap : tap + 1, :] * grad[11 - tap : 11 - tap + rows, :]
        dedge = dedge + weight[tap : tap + 1, :] * grad[3 - tap : 11 - tap, :]
        follow[tap] = masked[0:8, :]
    dedge_ref[...] = dedge
    dx_ref[...] = din[:, :inner].astype(bf16)
    dbc_ref[...] = din[:, inner:].astype(bf16)

    @pl.when(first)
    def _():
        tail_ref[...] = din[rows - 8 :, :]


def attention_kernel(
    low_ref, q_ref, do_ref, k0_ref, v0_ref, k1_ref, v1_ref, k2_ref, v2_ref, segc_ref, segr_ref,
    out_ref, dq_ref, dk0_ref, dv0_ref, dk1_ref, dv1_ref, dk2_ref, dv2_ref,
    dk_acc, dv_acc, acc, stats, dqt,
    *, scale,
):
    rows = q_ref.shape[0]
    blocks = rows // SPAN
    piece_refs = ((k2_ref, v2_ref), (k1_ref, v1_ref), (k0_ref, v0_ref))
    pieces = len(piece_refs)
    low = lane_low(SPAN)
    high = jnp.logical_not(low)
    zero = jnp.zeros((SPAN, LANES), bf16)
    top_rows = lax.broadcasted_iota(jnp.int32, (LANES, SPAN), 0) < ATT_DIM
    row = lax.broadcasted_iota(jnp.int32, (SPAN, SPAN), 0)
    col = lax.broadcasted_iota(jnp.int32, (SPAN, SPAN), 1)
    pick = (
        (lax.broadcasted_iota(jnp.int32, (8, LANES), 1) >= ATT_DIM)
        == (lax.broadcasted_iota(jnp.int32, (8, LANES), 0) == 1)
    ).astype(f32)
    dk_acc[...] = jnp.zeros_like(dk_acc)
    dv_acc[...] = jnp.zeros_like(dv_acc)

    def halves(value):
        return jnp.where(low, value, zero), jnp.where(high, value, zero)

    def allowed_at(piece, start, segr, block):
        same = segc_ref[pl.ds(piece * rows + start, SPAN), :] == segr
        if piece == pieces - 1:
            return same & (row + start <= col + block * SPAN)
        return same

    for block in range(blocks):
        q_rows = slice(block * SPAN, (block + 1) * SPAN)
        q_both = halves(q_ref[q_rows, :] * jnp.asarray(scale, bf16))
        do_full = do_ref[q_rows, :]
        do_both = halves(do_full)
        segr = segr_ref[:, q_rows]
        acc[...] = jnp.zeros_like(acc)
        stats[0:2, :] = jnp.full((2, SPAN), masked_score, f32)
        stats[2:4, :] = jnp.zeros((2, SPAN), f32)
        for piece in range(pieces):
            k_ref, v_ref = piece_refs[piece]
            stop = block + 1 if piece == pieces - 1 else blocks

            def forward_step(index, unused):
                start = pl.multiple_of(index * SPAN, SPAN)
                key = k_ref[pl.ds(start, SPAN), :]
                value_both = halves(v_ref[pl.ds(start, SPAN), :])
                allowed = allowed_at(piece, start, segr, block)
                added = jnp.zeros((LANES, SPAN), f32)
                shrink = []
                for head in range(2):
                    scores = jnp.where(allowed, dot_nt(key, q_both[head]), masked_score)
                    old_top = stats[head : head + 1, :]
                    new_top = jnp.maximum(old_top, jnp.max(scores, axis=0, keepdims=True))
                    weights = jnp.where(allowed, jnp.exp(scores - new_top), 0.0)
                    factor = jnp.exp(old_top - new_top)
                    stats[head : head + 1, :] = new_top
                    stats[2 + head : 3 + head, :] = stats[2 + head : 3 + head, :] * factor + jnp.sum(
                        weights, axis=0, keepdims=True
                    )
                    shrink.append(factor)
                    added = added + dot_tn(value_both[head], weights.astype(bf16))
                acc[...] = acc[...] * jnp.where(top_rows, shrink[0], shrink[1]) + added
                return unused

            lax.fori_loop(low_ref[block * pieces + piece], stop, forward_step, 0)
        inverse = [1.0 / stats[2 + head : 3 + head, :] for head in range(2)]
        attended = (acc[...] * jnp.where(top_rows, inverse[0], inverse[1])).T
        out_ref[q_rows, :] = attended.astype(bf16)
        delta = dot_nt(pick, do_full.astype(f32) * attended, highest)
        mass = [stats[head : head + 1, :] + jnp.log(stats[2 + head : 3 + head, :]) for head in range(2)]
        dqt[...] = jnp.zeros_like(dqt)
        for piece in range(pieces):
            k_ref, v_ref = piece_refs[piece]
            stop = block + 1 if piece == pieces - 1 else blocks

            def backward_step(index, unused):
                start = pl.multiple_of(index * SPAN, SPAN)
                key = k_ref[pl.ds(start, SPAN), :]
                value = v_ref[pl.ds(start, SPAN), :]
                key_both = halves(key)
                allowed = allowed_at(piece, start, segr, block)
                dk = jnp.zeros((SPAN, LANES), f32)
                dv = jnp.zeros((SPAN, LANES), f32)
                dq = jnp.zeros((LANES, SPAN), f32)
                for head in range(2):
                    scores = dot_nt(key, q_both[head])
                    weights = jnp.where(allowed, jnp.exp(scores - mass[head]), 0.0)
                    dweights = dot_nt(value, do_both[head])
                    dscores = (weights * (dweights - delta[head : head + 1, :])).astype(bf16)
                    dv = dv + dot_nn(weights.astype(bf16), do_both[head])
                    dk = dk + dot_nn(dscores, q_both[head])
                    dq = dq + dot_tn(key_both[head], dscores)
                where = pl.ds(piece * rows + start, SPAN)
                dk_acc[where, :] += dk
                dv_acc[where, :] += dv
                dqt[...] += dq
                return unused

            lax.fori_loop(low_ref[block * pieces + piece], stop, backward_step, 0)
        dq_ref[q_rows, :] = (dqt[...] * scale).T.astype(dq_ref.dtype)
    for piece, (dk_ref, dv_ref) in enumerate(((dk2_ref, dv2_ref), (dk1_ref, dv1_ref), (dk0_ref, dv0_ref))):
        dk_ref[...] = dk_acc[piece * rows : (piece + 1) * rows, :].astype(dk_ref.dtype)
        dv_ref[...] = dv_acc[piece * rows : (piece + 1) * rows, :].astype(dv_ref.dtype)


def from_behind(value, axis, by):
    count = lax.axis_size(axis)
    pairs = [(i, i + by) for i in range(count) if 0 <= i + by < count]
    return lax.ppermute(value, axis, pairs)


def params(**extra):
    return pltpu.CompilerParams(vmem_limit_bytes=VMEM_LIMIT, **extra)


def cost(flops, moved, transcendentals=0):
    return pl.CostEstimate(flops=int(flops), bytes_accessed=int(moved), transcendentals=int(transcendentals))


def fixed(shape):
    return pl.BlockSpec(shape, lambda *unused: (0,) * len(shape))


def ssd_specs(order, inner, bc_width, state_width):
    per = SPAN // 8
    channels = inner + bc_width

    def before(i):
        return jnp.maximum(order(i) * per - 1, 0)

    return [
        pl.BlockSpec((SPAN, inner), lambda i, *unused: (order(i), 1)),
        pl.BlockSpec((8, inner), lambda i, *unused: (before(i), 1)),
        pl.BlockSpec((SPAN, bc_width + LANES), lambda i, *unused: (order(i), 0)),
        pl.BlockSpec((8, bc_width + LANES), lambda i, *unused: (before(i), 0)),
        fixed((8, channels)),
        pl.BlockSpec((SPAN, 8), lambda i, *unused: (order(i), 0)),
        pl.BlockSpec((SPAN, 1), lambda i, *unused: (order(i), 0)),
        pl.BlockSpec((1, SPAN), lambda i, *unused: (0, order(i))),
    ]


def ssd_constant_specs(inner, channels):
    return [
        fixed((CONV, channels)),
        fixed((1, channels)),
        fixed((1, LANES)),
        fixed((1, LANES)),
        fixed((1, inner)),
        fixed((LANES, inner)),
        fixed((inner, LANES)),
    ]


def ssd_forward(prev, last, zx, bcs, edge, kept, segc, segr, constants, inner, width):
    rows = zx.shape[0]
    blocks = rows // SPAN
    channels = inner + 2 * width
    heads = inner // SSM_DIM
    order = lambda i: i
    return pl.pallas_call(
        ssd_forward_kernel,
        grid_spec=pltpu.PrefetchScalarGridSpec(
            num_scalar_prefetch=2,
            grid=(blocks,),
            in_specs=ssd_specs(order, inner, 2 * width, width) + ssd_constant_specs(inner, channels),
            out_specs=[
                pl.BlockSpec((SPAN, inner), lambda i, *unused: (i, 0)),
                pl.BlockSpec((SPAN, width), lambda i, *unused: (i, 0)),
                pl.BlockSpec((SPAN, LANES), lambda i, *unused: (i, 0)),
                pl.BlockSpec((inner, width), lambda i, *unused: (i, 0)),
                fixed((inner, width)),
                fixed((8, LANES)),
            ],
            scratch_shapes=[
                pltpu.VMEM((inner, width), f32),
                pltpu.VMEM((8, LANES), f32),
                pltpu.VMEM((SPAN + 8, channels), f32),
            ],
        ),
        out_shape=[
            jax.ShapeDtypeStruct((rows, inner), f32),
            jax.ShapeDtypeStruct((rows, width), bf16),
            jax.ShapeDtypeStruct((rows, LANES), f32),
            jax.ShapeDtypeStruct((blocks * inner, width), bf16),
            jax.ShapeDtypeStruct((inner, width), f32),
            jax.ShapeDtypeStruct((8, LANES), f32),
        ],
        compiler_params=params(),
        cost_estimate=cost(rows * SPAN * inner * 6, rows * inner * 12, rows * SPAN * heads),
        name="ssd_forward",
    )(prev, last, zx, zx, bcs, bcs, edge, kept, segc, segr, *constants)


def ssd_backward(prev, last, zx, bcs, edge, kept, segc, segr, dy, states, opened, entering, back_end, constants, inner, width):
    rows = zx.shape[0]
    blocks = rows // SPAN
    channels = inner + 2 * width
    heads = inner // SSM_DIM
    order = lambda i: blocks - 1 - i
    return pl.pallas_call(
        ssd_backward_kernel,
        grid_spec=pltpu.PrefetchScalarGridSpec(
            num_scalar_prefetch=2,
            grid=(blocks,),
            in_specs=ssd_specs(order, inner, 2 * width, width)
            + [
                pl.BlockSpec((SPAN, inner), lambda i, *unused: (order(i), 0)),
                pl.BlockSpec((inner, width), lambda i, *unused: (order(i), 0)),
                pl.BlockSpec((8, LANES), lambda i, *unused: (jnp.maximum(order(i) * (SPAN // 8) - 1, 0), 0)),
                fixed((inner, width)),
                fixed((inner, width)),
            ]
            + ssd_constant_specs(inner, channels),
            out_specs=[
                pl.BlockSpec((SPAN, inner), lambda i, *unused: (order(i), 0)),
                pl.BlockSpec((SPAN, 2 * width), lambda i, *unused: (order(i), 0)),
                pl.BlockSpec((SPAN, LANES), lambda i, *unused: (order(i), 0)),
                fixed((8, channels)),
                fixed((8, channels)),
                fixed((8, channels)),
                fixed((8, LANES)),
            ],
            scratch_shapes=[
                pltpu.VMEM((inner, width), f32),
                pltpu.VMEM((3, 8, channels), f32),
                pltpu.VMEM((SPAN + 8, channels), f32),
                pltpu.VMEM((SPAN + 16, channels), f32),
            ],
        ),
        out_shape=[
            jax.ShapeDtypeStruct((rows, inner), bf16),
            jax.ShapeDtypeStruct((rows, 2 * width), bf16),
            jax.ShapeDtypeStruct((rows, LANES), bf16),
            jax.ShapeDtypeStruct((8, channels), f32),
            jax.ShapeDtypeStruct((8, channels), f32),
            jax.ShapeDtypeStruct((8, channels), f32),
            jax.ShapeDtypeStruct((8, LANES), f32),
        ],
        compiler_params=params(),
        cost_estimate=cost(rows * SPAN * inner * 14, rows * inner * 16, rows * SPAN * heads),
        name="ssd_backward",
    )(prev, last, zx, zx, bcs, bcs, edge, kept, segc, segr, dy, states, opened, entering, back_end, *constants)


def gate_forward(y_zero, state_c, opened, entering, zx, gain, wide):
    rows, inner = y_zero.shape
    width = state_c.shape[1]
    return pl.pallas_call(
        gate_forward_kernel,
        grid=(rows // SPAN,),
        in_specs=[
            pl.BlockSpec((SPAN, inner), lambda i: (i, 0)),
            pl.BlockSpec((SPAN, width), lambda i: (i, 0)),
            pl.BlockSpec((SPAN, LANES), lambda i: (i, 0)),
            fixed((inner, width)),
            pl.BlockSpec((SPAN, inner), lambda i: (i, 0)),
            fixed((1, inner)),
            fixed((LANES, inner)),
        ],
        out_specs=[
            pl.BlockSpec((SPAN, inner), lambda i: (i, 0)),
            pl.BlockSpec((SPAN, inner), lambda i: (i, 0)),
            pl.BlockSpec((8, SPAN), lambda i: (0, i)),
        ],
        out_shape=[
            jax.ShapeDtypeStruct((rows, inner), f32),
            jax.ShapeDtypeStruct((rows, inner), bf16),
            jax.ShapeDtypeStruct((8, rows), f32),
        ],
        compiler_params=params(),
        cost_estimate=cost(rows * inner * width * 4, rows * inner * 14, rows * inner),
        name="gate_forward",
    )(y_zero, state_c, opened, entering, zx, gain, wide)


def gate_backward(back_gated, ssd_out, zx, coefficients, gain, state_c, opened, wide):
    rows, inner = ssd_out.shape
    width = state_c.shape[1]
    return pl.pallas_call(
        gate_backward_kernel,
        grid=(rows // SPAN,),
        in_specs=[
            pl.BlockSpec((SPAN, inner), lambda i: (i, 0)),
            pl.BlockSpec((SPAN, inner), lambda i: (i, 0)),
            pl.BlockSpec((SPAN, inner), lambda i: (i, 0)),
            pl.BlockSpec((SPAN, 8), lambda i: (i, 0)),
            fixed((1, inner)),
            pl.BlockSpec((SPAN, width), lambda i: (i, 0)),
            pl.BlockSpec((SPAN, LANES), lambda i: (i, 0)),
            fixed((LANES, inner)),
        ],
        out_specs=[
            pl.BlockSpec((SPAN, inner), lambda i: (i, 0)),
            pl.BlockSpec((SPAN, inner), lambda i: (i, 0)),
            pl.BlockSpec((SPAN, inner), lambda i: (i, 0)),
            fixed((1, inner)),
            fixed((inner, width)),
        ],
        out_shape=[
            jax.ShapeDtypeStruct((rows, inner), bf16),
            jax.ShapeDtypeStruct((rows, inner), bf16),
            jax.ShapeDtypeStruct((rows, inner), bf16),
            jax.ShapeDtypeStruct((1, inner), f32),
            jax.ShapeDtypeStruct((inner, width), f32),
        ],
        compiler_params=params(),
        cost_estimate=cost(rows * inner * width * 4, rows * inner * 18, rows * inner),
        name="gate_backward",
    )(back_gated, ssd_out, zx, coefficients, gain, state_c, opened, wide)


def attention(low_blocks, query_array, back_attended, pieces, segc, segr, att_pad, rows):
    pairs = att_pad // LANES
    scale = 1.0 / math.sqrt(ATT_DIM)
    count = len(pieces)

    def lane(offset):
        return pl.BlockSpec((rows, LANES), lambda p, *unused: (0, p + offset))

    in_specs = [lane(0), lane(0)]
    operands = [query_array, back_attended]
    for array, offset in pieces:
        in_specs += [lane(offset), lane(offset + pairs)]
        operands += [array, array]
    in_specs += [fixed((count * rows, 1)), fixed((1, rows))]
    shapes = [bf16, f32] + [f32, f32] + [bf16, bf16] * (count - 1)
    return pl.pallas_call(
        partial(attention_kernel, scale=scale),
        grid_spec=pltpu.PrefetchScalarGridSpec(
            num_scalar_prefetch=1,
            grid=(pairs,),
            in_specs=in_specs,
            out_specs=[lane(0)] * len(shapes),
            scratch_shapes=[
                pltpu.VMEM((count * rows, LANES), f32),
                pltpu.VMEM((count * rows, LANES), f32),
                pltpu.VMEM((LANES, SPAN), f32),
                pltpu.VMEM((8, SPAN), f32),
                pltpu.VMEM((LANES, SPAN), f32),
            ],
        ),
        out_shape=[jax.ShapeDtypeStruct((rows, att_pad), kind) for kind in shapes],
        compiler_params=params(),
        cost_estimate=cost(rows * rows * att_pad * 28, rows * att_pad * 30, rows * rows * pairs * 4),
        name="attention",
    )(low_blocks, *operands, segc, segr)


def fit(value, size, axis):
    if value.shape[axis] == size:
        return value
    widths = [(0, 0)] * value.ndim
    widths[axis] = (0, size - value.shape[axis])
    return jnp.pad(value, widths)


def head_gather(values):
    return lax.all_gather(values, "head", axis=1, tiled=True)


def head_scatter(values):
    return lax.psum_scatter(values, "head", scatter_dimension=1, tiled=True)


def seq_scatter(values):
    return lax.psum_scatter(values.astype(bf16), "seq", scatter_dimension=0, tiled=True).astype(f32)


def matmul(a, b, kind=f32):
    return jnp.dot(a, b, preferred_element_type=f32).astype(kind)


def matmul_nt(a, b, kind=f32):
    return lax.dot_general(a, b, (((1,), (1,)), ((), ())), preferred_element_type=f32).astype(kind)


def matmul_tn(a, b, kind=f32):
    return lax.dot_general(a, b, (((0,), (0,)), ((), ())), preferred_element_type=f32).astype(kind)


def per_device(
    tokens, segment_ids, first_gain, proj_zx, proj_bc, proj_step, conv_inner, conv_inner_bias,
    conv_state, conv_state_bias, step_bias, decay_log, skip_scale, gated_gain, proj_out,
    second_gain, proj_qkv, attention_out, cotangent,
):
    rows = tokens.shape[0]
    inner = proj_zx.shape[2]
    bc_width = proj_bc.shape[1]
    width = bc_width // 2
    channels = inner + bc_width
    heads = step_bias.shape[0]
    att = proj_qkv.shape[2]
    att_pad = -(-att // LANES) * LANES
    pairs = att_pad // LANES
    blocks = rows // SPAN
    reach = (DOC_MAX - 2) // rows + 1
    row_start = lax.axis_index("seq") * rows

    padded_seg = jnp.concatenate([jnp.full((reach * rows,), -1, jnp.int32), segment_ids])
    window = lax.dynamic_slice_in_dim(padded_seg, row_start, (reach + 1) * rows)
    local_seg = window[reach * rows :]
    shifted = window[reach * rows - (CONV - 1) :]
    kept = jnp.stack([(shifted[tap : tap + rows] == local_seg).astype(f32) for tap in range(CONV - 1)], axis=1)
    kept = fit(kept, 8, 1)
    span_prev = shifted[CONV - 2 :: SPAN][:blocks]
    span_last = local_seg[SPAN - 1 :: SPAN]
    segc_window = window[:, None]
    segc = local_seg[:, None]
    segr = local_seg[None, :]
    key_last = window[SPAN - 1 :: SPAN].reshape(reach + 1, blocks)
    query_first = local_seg[::SPAN]
    low_blocks = jnp.sum((key_last[None] < query_first[:, None, None]).astype(jnp.int32), axis=2).reshape(-1)

    owner = jnp.arange(inner, dtype=jnp.int32)[None, :] // SSM_DIM
    wide = (owner == jnp.arange(LANES, dtype=jnp.int32)[:, None]).astype(f32)
    tall = wide.T
    constants = (
        jnp.concatenate([conv_inner, conv_state], axis=1),
        jnp.concatenate([conv_inner_bias, conv_state_bias])[None],
        fit(step_bias[None], LANES, 1),
        fit(-jnp.exp(decay_log)[None], LANES, 1),
        jnp.repeat(skip_scale, SSM_DIM)[None],
        wide,
        tall,
    )
    zx_weight = proj_zx.reshape(D, 2 * inner)
    bcs_weight = jnp.concatenate([proj_bc, fit(proj_step, LANES, 1)], axis=1)
    qkv_weight = fit(proj_qkv, att_pad, 2).reshape(D, 3 * att_pad)
    att_weight = fit(attention_out, att_pad, 0)

    gains = lax.all_gather(jnp.stack([first_gain, second_gain]), "head", axis=1, tiled=True)
    token_full = head_gather(tokens).astype(f32)
    first_rms = lax.rsqrt(jnp.sum(token_full * token_full, axis=1) / D + epsilon)
    first_full = (token_full * first_rms[:, None] * gains[0]).astype(bf16)
    cot_full = head_gather(cotangent)
    zx = matmul(first_full, zx_weight)
    bcs = matmul(first_full, bcs_weight)
    edge_rows = jnp.concatenate([zx[rows - 8 :, inner:], bcs[rows - 8 :, :bc_width]], axis=1)
    edge = from_behind(edge_rows, "seq", 1)

    ssd_shared = (span_prev, span_last, zx, bcs, edge, kept, segc, segr)
    y_zero, state_c, opened, states, end_state, through = ssd_forward(*ssd_shared, constants, inner, width)
    through_rows = jnp.broadcast_to(jnp.repeat(through[0, :heads], SSM_DIM)[:, None], (inner, width))

    sent = end_state.astype(bf16)
    near = from_behind(sent, "seq", 1).astype(f32)
    packed = jnp.concatenate([sent, jnp.broadcast_to(through[0:1], (8, LANES)).astype(bf16)], axis=0)
    near_pack = from_behind(packed, "seq", 1).astype(f32)
    near = near_pack[:inner]
    near_through = jnp.repeat(near_pack[inner, :heads], SSM_DIM)[:, None]
    far = from_behind(sent, "seq", 2).astype(f32)
    entering = (near + near_through * far).astype(bf16)

    ssd_out, gated_raw, gate_sums = gate_forward(y_zero, state_c, opened, entering, zx, gated_gain[None], wide)
    gate_total = lax.psum(gate_sums[0], "head")
    gate_rms = lax.rsqrt(gate_total / INNER + epsilon)
    branch_part = matmul(gated_raw, proj_out, bf16)
    branch = head_scatter(branch_part).astype(f32) * gate_rms[:, None]
    hidden_zero = tokens.astype(f32)
    hidden_one = hidden_zero + branch
    second_total = lax.psum(jnp.sum(hidden_one * hidden_one, axis=1), "head")
    second_rms = lax.rsqrt(second_total / D + epsilon)
    second_full = head_gather((hidden_one * second_gain).astype(bf16))
    projected = (matmul(second_full, qkv_weight) * second_rms[:, None]).astype(bf16)
    key_value = projected[:, att_pad:]
    moved = [from_behind(key_value, "seq", back) for back in range(1, reach + 1)]

    back_attended = matmul_nt(cot_full, att_weight, bf16)
    pieces = [(projected, pairs)] + [(array, 0) for array in moved]
    attended, back_query, back_key, back_value, *back_moved = attention(
        low_blocks, projected, back_attended, pieces, segc_window, segr, att_pad, rows
    )
    output = (hidden_one + head_scatter(matmul(attended, att_weight, bf16)).astype(f32)).astype(bf16)
    grad_attention_out = matmul_tn(cot_full, attended[:, :att], bf16)

    for back in range(1, reach + 1):
        pair = jnp.concatenate(back_moved[2 * back - 2 : 2 * back], axis=1)
        pair = from_behind(pair, "seq", -back).astype(f32)
        back_key = back_key + pair[:, :att_pad]
        back_value = back_value + pair[:, att_pad:]
    back_projected = jnp.concatenate([back_query, back_key, back_value], axis=1).astype(bf16)
    back_second = head_scatter(matmul_nt(back_projected, qkv_weight, bf16)).astype(f32)
    second_dots = lax.psum(jnp.sum(back_projected.astype(f32) * projected.astype(f32), axis=1), "head")
    grad_qkv = matmul_tn(
        second_full, (back_projected.astype(f32) * second_rms[:, None]).astype(bf16), bf16
    )
    if att != att_pad:
        grad_qkv = grad_qkv.reshape(D, 3, att_pad)[:, :, :att].reshape(D, 3 * att)
    normed_one = hidden_one * second_rms[:, None]
    grad_second_gain = jnp.sum(normed_one * back_second, axis=0)
    back_hidden_one = (
        cotangent.astype(f32)
        + second_rms[:, None] * second_gain * back_second
        - hidden_one * (second_rms * second_rms / D * second_dots)[:, None]
    )
    back_low = back_hidden_one.astype(bf16)
    back_branch = head_gather(back_low)
    back_gated = matmul_nt(back_branch, proj_out, bf16)
    gate_dots = lax.psum(jnp.sum(back_low.astype(f32) * branch, axis=1), "head")
    coefficients = fit(jnp.stack([gate_rms, gate_rms * gate_rms / INNER * gate_dots], axis=1), 8, 1)
    dy, back_z, gated, grad_gated_gain, back_entering = gate_backward(
        back_gated, ssd_out, zx, coefficients, gated_gain[None], state_c, opened, wide
    )
    grad_out = matmul_tn(back_branch, gated, bf16)

    back_sent = back_entering.astype(bf16)
    back_pack = jnp.concatenate([back_sent, jnp.broadcast_to(through[0:1], (8, LANES)).astype(bf16)], axis=0)
    back_near_pack = from_behind(back_pack, "seq", -1).astype(f32)
    back_far = from_behind(back_sent, "seq", -2).astype(f32)
    back_near_through = jnp.repeat(back_near_pack[inner, :heads], SSM_DIM)[:, None]
    back_end = back_near_pack[:inner] + back_near_through * back_far

    back_x, back_bc, back_step, tail_rows, back_edge, grad_conv, grad_heads = ssd_backward(
        *ssd_shared, dy, states, opened, entering, back_end, constants, inner, width
    )
    tail_rows = (tail_rows + from_behind(back_edge, "seq", -1)).astype(bf16)
    back_x = lax.dynamic_update_slice(back_x, tail_rows[:, :inner], (rows - 8, 0))
    back_bc = lax.dynamic_update_slice(back_bc, tail_rows[:, inner:], (rows - 8, 0))

    first_part = (
        matmul_nt(back_z, zx_weight[:, :inner])
        + matmul_nt(back_x, zx_weight[:, inner:])
        + matmul_nt(back_bc, proj_bc)
        + matmul_nt(back_step, bcs_weight[:, bc_width:])
    ).astype(bf16)
    back_first = head_scatter(first_part).astype(f32)
    first_dots = lax.psum(
        jnp.sum(back_z.astype(f32) * zx[:, :inner], axis=1)
        + jnp.sum(back_x.astype(f32) * zx[:, inner:], axis=1)
        + jnp.sum(back_bc.astype(f32) * bcs[:, :bc_width], axis=1)
        + jnp.sum(back_step.astype(f32) * bcs[:, bc_width:], axis=1),
        "head",
    )
    grad_zx_gate = matmul_tn(first_full, back_z, bf16)
    grad_zx_inner = matmul_tn(first_full, back_x, bf16)
    grad_bc = matmul_tn(first_full, back_bc, bf16)
    grad_step = matmul_tn(first_full, back_step)[:, :heads].astype(bf16)
    grad_first_gain = jnp.sum(hidden_zero * first_rms[:, None] * back_first, axis=0)
    grad_tokens = (
        back_hidden_one
        + first_rms[:, None] * first_gain * back_first
        - hidden_zero * (first_rms * first_rms / D * first_dots)[:, None]
    ).astype(bf16)

    wide_qkv = seq_scatter(grad_qkv).reshape(-1, 3, att)
    wide_att = seq_scatter(grad_attention_out).T
    wide_out = seq_scatter(grad_out).T
    wide_zx = jnp.stack([seq_scatter(grad_zx_gate), seq_scatter(grad_zx_inner)], axis=1)
    wide_step = seq_scatter(grad_step)
    both = ("seq", "head")
    shared_bc = lax.psum_scatter(grad_bc, both, scatter_dimension=1, tiled=True).astype(f32)
    shared_conv = lax.psum_scatter(grad_conv[:5, inner:], both, scatter_dimension=1, tiled=True)
    small = lax.psum(
        (
            grad_first_gain,
            grad_conv[:5, :inner],
            grad_heads[:3, :heads],
            grad_gated_gain[0],
            grad_second_gain,
        ),
        "seq",
    )
    return (
        output,
        grad_tokens,
        small[0],
        wide_zx,
        shared_bc,
        wide_step,
        small[1][:4],
        small[1][4],
        shared_conv[:4],
        shared_conv[4],
        small[2][0],
        small[2][1],
        small[2][2],
        small[3],
        wide_out,
        small[4],
        wide_qkv,
        wide_att,
    )


def solution(mesh):
    placed = (
        P("seq", "head"),
        P(),
        P("head"),
        P(None, None, "head"),
        P(),
        P(None, "head"),
        P(None, "head"),
        P("head"),
        P(),
        P(),
        P("head"),
        P("head"),
        P("head"),
        P("head"),
        P("head", None),
        P("head"),
        P(None, None, "head"),
        P("head", None),
        P("seq", "head"),
    )
    return jax.shard_map(
        per_device,
        mesh=mesh,
        in_specs=placed,
        out_specs=(
            P("seq", "head"),
            P("seq", "head"),
            P("head"),
            P("seq", None, "head"),
            P(None, ("seq", "head")),
            P("seq", "head"),
            P(None, "head"),
            P("head"),
            P(None, ("seq", "head")),
            P(("seq", "head")),
            P("head"),
            P("head"),
            P("head"),
            P("head"),
            P("head", "seq"),
            P("head"),
            P("seq", None, "head"),
            P("head", "seq"),
        ),
        check_vma=False,
    )
```

```python
from functools import partial
import math

import jax
import jax.numpy as jnp
from jax import lax
from jax.experimental import pallas as pl
from jax.experimental.pallas import tpu as pltpu
from jax.sharding import PartitionSpec as P

D = 1536
ATT_DIM = 64
SSM_DIM = 64
SPAN = 256
CONV = 4
DOC_MAX = 2000
INNER = 3072
LANES = 128

epsilon = 1e-05
highest = lax.Precision.HIGHEST
f32 = jnp.float32
bf16 = jnp.bfloat16
masked_score = -1e30
VMEM_LIMIT = 60 * 1024 * 1024


def dot_nn(a, b, precision=None):
    return lax.dot_general(a, b, (((1,), (0,)), ((), ())), precision=precision, preferred_element_type=f32)


def dot_nt(a, b, precision=None):
    return lax.dot_general(a, b, (((1,), (1,)), ((), ())), precision=precision, preferred_element_type=f32)


def dot_tn(a, b, precision=None):
    return lax.dot_general(a, b, (((0,), (0,)), ((), ())), precision=precision, preferred_element_type=f32)


def softplus(x):
    return jnp.maximum(x, 0.0) + jnp.log1p(jnp.exp(-jnp.abs(x)))


def sigmoid(x):
    return 1.0 / (1.0 + jnp.exp(-x))


def lane_low(rows):
    return lax.broadcasted_iota(jnp.int32, (rows, LANES), 1) < SSM_DIM


def conv_rows(buf, weight, bias, kept, rows):
    summed = bias + weight[3:4, :] * buf[8 : 8 + rows, :]
    for tap in range(3):
        summed = summed + weight[tap : tap + 1, :] * (buf[5 + tap : 5 + tap + rows, :] * kept[:, tap : tap + 1])
    return summed


def fill_conv(buf, chunk, x_ref, xprev_ref, bcs_ref, bprev_ref, edge_ref, inner, rows):
    buf[8 : 8 + rows, :inner] = x_ref[...]
    buf[8 : 8 + rows, inner:] = bcs_ref[:, : buf.shape[1] - inner]

    @pl.when(chunk == 0)
    def _():
        buf[0:8, :] = edge_ref[...]

    @pl.when(chunk > 0)
    def _():
        buf[0:8, :inner] = xprev_ref[...]
        buf[0:8, inner:] = bprev_ref[:, : buf.shape[1] - inner]


def span_terms(bcs_ref, bc_width, bias_ref, rate_ref, segc_ref, segr_ref, prev, last, rows):
    raw = bcs_ref[:, bc_width:] + bias_ref[...]
    step = softplus(raw)
    decay = rate_ref[...] * step
    row = lax.broadcasted_iota(jnp.int32, (rows, rows), 0)
    col = lax.broadcasted_iota(jnp.int32, (rows, rows), 1)
    causal = row >= col
    tri = causal.astype(f32)
    cum = dot_nn(tri, decay, highest)
    segc = segc_ref[...]
    allowed = (segc == segr_ref[...]) & causal
    opened = (segc == prev).astype(f32)
    closing = (segc == last).astype(f32)
    last_cum = cum[rows - 1 : rows, :]
    enter = jnp.exp(cum) * opened
    tail = jnp.exp(last_cum - cum) * closing
    through = jnp.exp(last_cum) * (last == prev).astype(f32)
    return raw, step, decay, cum, tri, allowed, enter, tail, last_cum, through


def ssd_forward_kernel(
    prev_ref, last_ref, x_ref, xprev_ref, bcs_ref, bprev_ref, edge_ref, kept_ref, segc_ref, segr_ref,
    weight_ref, cbias_ref, bias_ref, rate_ref, skip_ref, wide_ref, tall_ref,
    y_ref, c_ref, open_ref, states_ref, end_ref, through_ref,
    state, base, buf,
):
    chunk = pl.program_id(0)
    rows = x_ref.shape[0]
    inner = x_ref.shape[1]
    width = c_ref.shape[1]
    heads = inner // SSM_DIM

    @pl.when(chunk == 0)
    def _():
        state[...] = jnp.zeros_like(state)
        base[...] = jnp.zeros_like(base)

    fill_conv(buf, chunk, x_ref, xprev_ref, bcs_ref, bprev_ref, edge_ref, inner, rows)
    pre = conv_rows(buf, weight_ref[...], cbias_ref[...], kept_ref[...], rows)
    conv = pre * sigmoid(pre)
    values = conv[:, :inner]
    b_low = conv[:, inner : inner + width].astype(bf16)
    c_low = conv[:, inner + width :].astype(bf16)
    prev, last, prev_dev = prev_ref[chunk], last_ref[chunk], prev_ref[0]
    raw, step, decay, cum, tri, allowed, enter, tail, last_cum, through = span_terms(
        bcs_ref, 2 * width, bias_ref, rate_ref, segc_ref, segr_ref, prev, last, rows
    )
    cum_t = cum.T
    inter = jnp.where(allowed, dot_nt(c_low, b_low), 0.0)
    wide = wide_ref[...]
    scaled = values * dot_nn(step, wide, highest)
    scaled_low = scaled.astype(bf16)
    old = state[...]
    old_low = old.astype(bf16)
    states_ref[...] = old_low
    c_ref[...] = c_low
    carried = dot_nt(c_low, old_low) * dot_nn(enter, wide, highest) + skip_ref[...] * values
    low = lane_low(rows)
    for pair in range(heads // 2):
        cols = slice(pair * LANES, (pair + 1) * LANES)
        both = []
        for head in (2 * pair, 2 * pair + 1):
            spread = jnp.exp(jnp.minimum(cum[:, head : head + 1] - cum_t[head : head + 1, :], 0.0))
            both.append(dot_nn((inter * spread).astype(bf16), scaled_low[:, cols]))
        y_ref[:, cols] = jnp.where(low, both[0], both[1]) + carried[:, cols]
    fresh = dot_tn((scaled * dot_nn(tail, wide, highest)).astype(bf16), b_low)
    through_rows = jnp.broadcast_to(through, (8, LANES))
    column = dot_nt(tall_ref[...], through_rows, highest)[:, 0:1]
    new = old * column + fresh
    state[...] = new
    end_ref[...] = new
    total = base[0:1, :]
    open_ref[...] = jnp.exp(total + cum) * (segc_ref[...] == prev_dev).astype(f32)
    base[...] = jnp.broadcast_to(total + last_cum, base.shape)
    through_ref[...] = jnp.broadcast_to(
        jnp.exp(total + last_cum) * (last == prev_dev).astype(f32), through_ref.shape
    )


def gate_forward_kernel(y_ref, c_ref, open_ref, enter_ref, z_ref, gain_ref, wide_ref, ssd_ref, out_ref, sum_ref):
    ssd = y_ref[...] + dot_nt(c_ref[...], enter_ref[...]) * dot_nn(open_ref[...], wide_ref[...], highest)
    z = z_ref[...]
    mixed = ssd * (z * sigmoid(z))
    ssd_ref[...] = ssd
    out_ref[...] = (mixed * gain_ref[...]).astype(bf16)
    sum_ref[...] = dot_nt(jnp.ones((8, mixed.shape[1]), f32), mixed * mixed, highest)


def gate_backward_kernel(
    bg_ref, ssd_ref, z_ref, rc_ref, gain_ref, c_ref, open_ref, wide_ref,
    dy_ref, gz_ref, gated_ref, ggain_ref, enter_ref,
):
    @pl.when(pl.program_id(0) == 0)
    def _():
        ggain_ref[...] = jnp.zeros_like(ggain_ref)
        enter_ref[...] = jnp.zeros_like(enter_ref)

    ssd = ssd_ref[...]
    z = z_ref[...]
    sig = sigmoid(z)
    gate = z * sig
    mixed = ssd * gate
    rms = rc_ref[:, 0:1]
    back = bg_ref[...].astype(f32)
    normed = mixed * rms
    gained = back * gain_ref[...]
    g_mixed = gained * rms - mixed * rc_ref[:, 1:2]
    gated_ref[...] = (normed * gain_ref[...]).astype(bf16)
    ggain_ref[...] += jnp.sum(normed * back, axis=0, keepdims=True)
    dy = (g_mixed * gate).astype(bf16)
    dy_ref[...] = dy
    gz_ref[...] = (g_mixed * ssd * (sig + gate * (1.0 - sig))).astype(bf16)
    opened = (dy.astype(f32) * dot_nn(open_ref[...], wide_ref[...], highest)).astype(bf16)
    enter_ref[...] += dot_tn(opened, c_ref[...])


def ssd_backward_kernel(
    prev_ref, last_ref, x_ref, xprev_ref, bcs_ref, bprev_ref, edge_ref, kept_ref, segc_ref, segr_ref,
    dy_ref, states_ref, openprev_ref, enter_ref, back_ref,
    weight_ref, cbias_ref, bias_ref, rate_ref, skip_ref, wide_ref, tall_ref,
    dx_ref, dbc_ref, dstep_ref, tail_ref, dedge_ref, dconv_ref, dhead_ref,
    dstate, follow, buf, grad,
):
    rows = x_ref.shape[0]
    inner = x_ref.shape[1]
    width = states_ref.shape[1]
    heads = inner // SSM_DIM
    first = pl.program_id(0) == 0
    chunk = pl.num_programs(0) - 1 - pl.program_id(0)

    @pl.when(first)
    def _():
        dstate[...] = back_ref[...]
        follow[...] = jnp.zeros_like(follow)
        dconv_ref[...] = jnp.zeros_like(dconv_ref)
        dhead_ref[...] = jnp.zeros_like(dhead_ref)

    fill_conv(buf, chunk, x_ref, xprev_ref, bcs_ref, bprev_ref, edge_ref, inner, rows)
    weight = weight_ref[...]
    kept = kept_ref[...]
    pre = conv_rows(buf, weight, cbias_ref[...], kept, rows)
    sig = sigmoid(pre)
    conv = pre * sig
    slope = sig + conv * (1.0 - sig)
    values = conv[:, :inner]
    b_low = conv[:, inner : inner + width].astype(bf16)
    c_low = conv[:, inner + width :].astype(bf16)
    prev, last = prev_ref[chunk], last_ref[chunk]
    raw, step, decay, cum, tri, allowed, enter, tail, last_cum, through = span_terms(
        bcs_ref, 2 * width, bias_ref, rate_ref, segc_ref, segr_ref, prev, last, rows
    )
    cum_t = cum.T
    inter = jnp.where(allowed, dot_nt(c_low, b_low), 0.0)
    wide = wide_ref[...]
    tall = tall_ref[...]
    step_wide = dot_nn(step, wide, highest)
    enter_wide = dot_nn(enter, wide, highest)
    tail_wide = dot_nn(tail, wide, highest)
    scaled_low = (values * step_wide).astype(bf16)
    scaled = scaled_low.astype(f32)
    dy_low = dy_ref[...]
    dy = dy_low.astype(f32)
    reach = jnp.where(chunk == 0, jnp.ones((8, LANES), f32), jnp.broadcast_to(openprev_ref[7:8, :], (8, LANES)))
    old = states_ref[...].astype(f32) + dot_nt(tall, reach, highest)[:, 0:1] * enter_ref[...].astype(f32)
    old_low = old.astype(bf16)
    dnew = dstate[...]
    dnew_low = dnew.astype(bf16)
    dy_enter = (dy * enter_wide).astype(bf16)
    from_state = dot_nt(c_low, old_low) * enter_wide
    to_state = dot_nt(b_low, dnew_low) * tail_wide
    dc = dot_nn(dy_enter, old_low)
    db = dot_nn((scaled * tail_wide).astype(bf16), dnew_low)
    through_column = dot_nt(tall, jnp.broadcast_to(through, (8, LANES)), highest)[:, 0:1]
    state_dots = jnp.sum(dnew * old, axis=1, keepdims=True) * through_column
    through_sum = jnp.sum(tall * state_dots, axis=0, keepdims=True)
    dstate[...] = dnew * through_column + dot_tn(dy_enter, c_low)
    low = lane_low(rows)
    mixed_grad = jnp.zeros((rows, rows), f32)
    within_parts = []
    dscaled_parts = []
    for pair in range(heads // 2):
        cols = slice(pair * LANES, (pair + 1) * LANES)
        scaled_pair = scaled_low[:, cols]
        dy_pair = dy_low[:, cols]
        ahead = []
        behind = []
        for index in range(2):
            head = 2 * pair + index
            spread = jnp.exp(jnp.minimum(cum[:, head : head + 1] - cum_t[head : head + 1, :], 0.0))
            mixing = (inter * spread).astype(bf16)
            dy_one = jnp.where(low if index == 0 else jnp.logical_not(low), dy_pair, jnp.zeros_like(dy_pair))
            mixed_grad = mixed_grad + dot_nt(dy_one, scaled_pair) * spread
            ahead.append(dot_nn(mixing, scaled_pair))
            behind.append(dot_tn(mixing, dy_pair))
        within_parts.append(jnp.where(low, ahead[0], ahead[1]))
        dscaled_parts.append(jnp.where(low, behind[0], behind[1]))
    within = jnp.concatenate(within_parts, axis=1)
    dscaled = jnp.concatenate(dscaled_parts, axis=1)
    mixed_low = jnp.where(allowed, mixed_grad, 0.0).astype(bf16)
    dc = dc + dot_nn(mixed_low, b_low)
    db = db + dot_tn(mixed_low, c_low)
    fresh_dots = dot_nn(scaled * to_state, tall, highest)
    dcum = dot_nn(dy * (within + from_state) - scaled * dscaled, tall, highest) - fresh_dots
    tail_sum = jnp.sum(fresh_dots, axis=0, keepdims=True) + through_sum
    ddecay = dot_tn(tri, dcum, highest) + tail_sum
    dscaled = dscaled + to_state
    dvalues = step_wide * dscaled + skip_ref[...] * dy
    dstep = dot_nn(dscaled * values, tall, highest) + ddecay * rate_ref[...]
    draw = dstep * sigmoid(raw)
    dskip = jnp.sum(dot_nn(dy * values, tall, highest), axis=0, keepdims=True)
    dhead_ref[0:1, :] += jnp.sum(draw, axis=0, keepdims=True)
    dhead_ref[1:2, :] += jnp.sum(ddecay * decay, axis=0, keepdims=True)
    dhead_ref[2:3, :] += dskip
    dstep_ref[...] = draw.astype(bf16)
    dpre = jnp.concatenate([dvalues, db, dc], axis=1) * slope
    din = weight[3:4, :] * dpre
    dconv_ref[3:4, :] += jnp.sum(dpre * buf[8 : 8 + rows, :], axis=0, keepdims=True)
    dconv_ref[4:5, :] += jnp.sum(dpre, axis=0, keepdims=True)
    dedge = jnp.zeros((8, dpre.shape[1]), f32)
    for tap in range(3):
        masked = dpre * kept[:, tap : tap + 1]
        dconv_ref[tap : tap + 1, :] += jnp.sum(masked * buf[5 + tap : 5 + tap + rows, :], axis=0, keepdims=True)
        grad[0:8, :] = jnp.zeros((8, dpre.shape[1]), f32)
        grad[8 : 8 + rows, :] = masked
        grad[8 + rows :, :] = follow[tap]
        din = din + weight[tap : tap + 1, :] * grad[11 - tap : 11 - tap + rows, :]
        dedge = dedge + weight[tap : tap + 1, :] * grad[3 - tap : 11 - tap, :]
        follow[tap] = masked[0:8, :]
    dedge_ref[...] = dedge
    dx_ref[...] = din[:, :inner].astype(bf16)
    dbc_ref[...] = din[:, inner:].astype(bf16)

    @pl.when(first)
    def _():
        tail_ref[...] = din[rows - 8 :, :]


def attention_kernel(
    low_ref, q_ref, do_ref, k0_ref, v0_ref, k1_ref, v1_ref, k2_ref, v2_ref, segc_ref, segr_ref,
    out_ref, dq_ref, dk0_ref, dv0_ref, dk1_ref, dv1_ref, dk2_ref, dv2_ref,
    dk_acc, dv_acc, acc, stats, dqt,
    *, scale,
):
    rows = q_ref.shape[0]
    blocks = rows // SPAN
    piece_refs = ((k2_ref, v2_ref), (k1_ref, v1_ref), (k0_ref, v0_ref))
    pieces = len(piece_refs)
    low = lane_low(SPAN)
    high = jnp.logical_not(low)
    zero = jnp.zeros((SPAN, LANES), bf16)
    top_rows = lax.broadcasted_iota(jnp.int32, (LANES, SPAN), 0) < ATT_DIM
    row = lax.broadcasted_iota(jnp.int32, (SPAN, SPAN), 0)
    col = lax.broadcasted_iota(jnp.int32, (SPAN, SPAN), 1)
    pick = (
        (lax.broadcasted_iota(jnp.int32, (8, LANES), 1) >= ATT_DIM)
        == (lax.broadcasted_iota(jnp.int32, (8, LANES), 0) == 1)
    ).astype(f32)
    dk_acc[...] = jnp.zeros_like(dk_acc)
    dv_acc[...] = jnp.zeros_like(dv_acc)

    def halves(value):
        return jnp.where(low, value, zero), jnp.where(high, value, zero)

    def allowed_at(piece, start, segr, block):
        same = segc_ref[pl.ds(piece * rows + start, SPAN), :] == segr
        if piece == pieces - 1:
            return same & (row + start <= col + block * SPAN)
        return same

    for block in range(blocks):
        q_rows = slice(block * SPAN, (block + 1) * SPAN)
        q_both = halves(q_ref[q_rows, :] * jnp.asarray(scale, bf16))
        do_full = do_ref[q_rows, :]
        do_both = halves(do_full)
        segr = segr_ref[:, q_rows]
        acc[...] = jnp.zeros_like(acc)
        stats[0:2, :] = jnp.full((2, SPAN), masked_score, f32)
        stats[2:4, :] = jnp.zeros((2, SPAN), f32)
        for piece in range(pieces):
            k_ref, v_ref = piece_refs[piece]
            stop = block + 1 if piece == pieces - 1 else blocks

            def forward_step(index, unused):
                start = pl.multiple_of(index * SPAN, SPAN)
                key = k_ref[pl.ds(start, SPAN), :]
                value_both = halves(v_ref[pl.ds(start, SPAN), :])
                allowed = allowed_at(piece, start, segr, block)
                added = jnp.zeros((LANES, SPAN), f32)
                shrink = []
                for head in range(2):
                    scores = jnp.where(allowed, dot_nt(key, q_both[head]), masked_score)
                    old_top = stats[head : head + 1, :]
                    new_top = jnp.maximum(old_top, jnp.max(scores, axis=0, keepdims=True))
                    weights = jnp.where(allowed, jnp.exp(scores - new_top), 0.0)
                    factor = jnp.exp(old_top - new_top)
                    stats[head : head + 1, :] = new_top
                    stats[2 + head : 3 + head, :] = stats[2 + head : 3 + head, :] * factor + jnp.sum(
                        weights, axis=0, keepdims=True
                    )
                    shrink.append(factor)
                    added = added + dot_tn(value_both[head], weights.astype(bf16))
                acc[...] = acc[...] * jnp.where(top_rows, shrink[0], shrink[1]) + added
                return unused

            lax.fori_loop(low_ref[block * pieces + piece], stop, forward_step, 0)
        inverse = [1.0 / stats[2 + head : 3 + head, :] for head in range(2)]
        attended = (acc[...] * jnp.where(top_rows, inverse[0], inverse[1])).T
        out_ref[q_rows, :] = attended.astype(bf16)
        delta = dot_nt(pick, do_full.astype(f32) * attended, highest)
        mass = [stats[head : head + 1, :] + jnp.log(stats[2 + head : 3 + head, :]) for head in range(2)]
        dqt[...] = jnp.zeros_like(dqt)
        for piece in range(pieces):
            k_ref, v_ref = piece_refs[piece]
            stop = block + 1 if piece == pieces - 1 else blocks

            def backward_step(index, unused):
                start = pl.multiple_of(index * SPAN, SPAN)
                key = k_ref[pl.ds(start, SPAN), :]
                value = v_ref[pl.ds(start, SPAN), :]
                key_both = halves(key)
                allowed = allowed_at(piece, start, segr, block)
                dk = jnp.zeros((SPAN, LANES), f32)
                dv = jnp.zeros((SPAN, LANES), f32)
                dq = jnp.zeros((LANES, SPAN), f32)
                for head in range(2):
                    scores = dot_nt(key, q_both[head])
                    weights = jnp.where(allowed, jnp.exp(scores - mass[head]), 0.0)
                    dweights = dot_nt(value, do_both[head])
                    dscores = (weights * (dweights - delta[head : head + 1, :])).astype(bf16)
                    dv = dv + dot_nn(weights.astype(bf16), do_both[head])
                    dk = dk + dot_nn(dscores, q_both[head])
                    dq = dq + dot_tn(key_both[head], dscores)
                where = pl.ds(piece * rows + start, SPAN)
                dk_acc[where, :] += dk
                dv_acc[where, :] += dv
                dqt[...] += dq
                return unused

            lax.fori_loop(low_ref[block * pieces + piece], stop, backward_step, 0)
        dq_ref[q_rows, :] = (dqt[...] * scale).T.astype(dq_ref.dtype)
    for piece, (dk_ref, dv_ref) in enumerate(((dk2_ref, dv2_ref), (dk1_ref, dv1_ref), (dk0_ref, dv0_ref))):
        dk_ref[...] = dk_acc[piece * rows : (piece + 1) * rows, :].astype(dk_ref.dtype)
        dv_ref[...] = dv_acc[piece * rows : (piece + 1) * rows, :].astype(dv_ref.dtype)


def from_behind(value, axis, by):
    count = lax.axis_size(axis)
    pairs = [(i, i + by) for i in range(count) if 0 <= i + by < count]
    return lax.ppermute(value, axis, pairs)


def params(**extra):
    return pltpu.CompilerParams(vmem_limit_bytes=VMEM_LIMIT, **extra)


def cost(flops, moved, transcendentals=0):
    return pl.CostEstimate(flops=int(flops), bytes_accessed=int(moved), transcendentals=int(transcendentals))


def fixed(shape):
    return pl.BlockSpec(shape, lambda *unused: (0,) * len(shape))


def ssd_specs(order, inner, bc_width, state_width):
    per = SPAN // 8
    channels = inner + bc_width

    def before(i):
        return jnp.maximum(order(i) * per - 1, 0)

    return [
        pl.BlockSpec((SPAN, inner), lambda i, *unused: (order(i), 0)),
        pl.BlockSpec((8, inner), lambda i, *unused: (before(i), 0)),
        pl.BlockSpec((SPAN, bc_width + LANES), lambda i, *unused: (order(i), 0)),
        pl.BlockSpec((8, bc_width + LANES), lambda i, *unused: (before(i), 0)),
        fixed((8, channels)),
        pl.BlockSpec((SPAN, 8), lambda i, *unused: (order(i), 0)),
        pl.BlockSpec((SPAN, 1), lambda i, *unused: (order(i), 0)),
        pl.BlockSpec((1, SPAN), lambda i, *unused: (0, order(i))),
    ]


def ssd_constant_specs(inner, channels):
    return [
        fixed((CONV, channels)),
        fixed((1, channels)),
        fixed((1, LANES)),
        fixed((1, LANES)),
        fixed((1, inner)),
        fixed((LANES, inner)),
        fixed((inner, LANES)),
    ]


def ssd_forward(prev, last, zx, bcs, edge, kept, segc, segr, constants, inner, width):
    rows = zx.shape[0]
    blocks = rows // SPAN
    channels = inner + 2 * width
    heads = inner // SSM_DIM
    order = lambda i: i
    return pl.pallas_call(
        ssd_forward_kernel,
        grid_spec=pltpu.PrefetchScalarGridSpec(
            num_scalar_prefetch=2,
            grid=(blocks,),
            in_specs=ssd_specs(order, inner, 2 * width, width) + ssd_constant_specs(inner, channels),
            out_specs=[
                pl.BlockSpec((SPAN, inner), lambda i, *unused: (i, 0)),
                pl.BlockSpec((SPAN, width), lambda i, *unused: (i, 0)),
                pl.BlockSpec((SPAN, LANES), lambda i, *unused: (i, 0)),
                pl.BlockSpec((inner, width), lambda i, *unused: (i, 0)),
                fixed((inner, width)),
                fixed((8, LANES)),
            ],
            scratch_shapes=[
                pltpu.VMEM((inner, width), f32),
                pltpu.VMEM((8, LANES), f32),
                pltpu.VMEM((SPAN + 8, channels), f32),
            ],
        ),
        out_shape=[
            jax.ShapeDtypeStruct((rows, inner), f32),
            jax.ShapeDtypeStruct((rows, width), bf16),
            jax.ShapeDtypeStruct((rows, LANES), f32),
            jax.ShapeDtypeStruct((blocks * inner, width), bf16),
            jax.ShapeDtypeStruct((inner, width), f32),
            jax.ShapeDtypeStruct((8, LANES), f32),
        ],
        compiler_params=params(),
        cost_estimate=cost(rows * SPAN * inner * 6, rows * inner * 12, rows * SPAN * heads),
        name="ssd_forward",
    )(prev, last, zx, zx, bcs, bcs, edge, kept, segc, segr, *constants)


def ssd_backward(prev, last, zx, bcs, edge, kept, segc, segr, dy, states, opened, entering, back_end, constants, inner, width):
    rows = zx.shape[0]
    blocks = rows // SPAN
    channels = inner + 2 * width
    heads = inner // SSM_DIM
    order = lambda i: blocks - 1 - i
    return pl.pallas_call(
        ssd_backward_kernel,
        grid_spec=pltpu.PrefetchScalarGridSpec(
            num_scalar_prefetch=2,
            grid=(blocks,),
            in_specs=ssd_specs(order, inner, 2 * width, width)
            + [
                pl.BlockSpec((SPAN, inner), lambda i, *unused: (order(i), 0)),
                pl.BlockSpec((inner, width), lambda i, *unused: (order(i), 0)),
                pl.BlockSpec((8, LANES), lambda i, *unused: (jnp.maximum(order(i) * (SPAN // 8) - 1, 0), 0)),
                fixed((inner, width)),
                fixed((inner, width)),
            ]
            + ssd_constant_specs(inner, channels),
            out_specs=[
                pl.BlockSpec((SPAN, inner), lambda i, *unused: (order(i), 0)),
                pl.BlockSpec((SPAN, 2 * width), lambda i, *unused: (order(i), 0)),
                pl.BlockSpec((SPAN, LANES), lambda i, *unused: (order(i), 0)),
                fixed((8, channels)),
                fixed((8, channels)),
                fixed((8, channels)),
                fixed((8, LANES)),
            ],
            scratch_shapes=[
                pltpu.VMEM((inner, width), f32),
                pltpu.VMEM((3, 8, channels), f32),
                pltpu.VMEM((SPAN + 8, channels), f32),
                pltpu.VMEM((SPAN + 16, channels), f32),
            ],
        ),
        out_shape=[
            jax.ShapeDtypeStruct((rows, inner), bf16),
            jax.ShapeDtypeStruct((rows, 2 * width), bf16),
            jax.ShapeDtypeStruct((rows, LANES), bf16),
            jax.ShapeDtypeStruct((8, channels), f32),
            jax.ShapeDtypeStruct((8, channels), f32),
            jax.ShapeDtypeStruct((8, channels), f32),
            jax.ShapeDtypeStruct((8, LANES), f32),
        ],
        compiler_params=params(),
        cost_estimate=cost(rows * SPAN * inner * 14, rows * inner * 16, rows * SPAN * heads),
        name="ssd_backward",
    )(prev, last, zx, zx, bcs, bcs, edge, kept, segc, segr, dy, states, opened, entering, back_end, *constants)


def gate_forward(y_zero, state_c, opened, entering, zx, gain, wide):
    rows, inner = y_zero.shape
    width = state_c.shape[1]
    return pl.pallas_call(
        gate_forward_kernel,
        grid=(rows // SPAN,),
        in_specs=[
            pl.BlockSpec((SPAN, inner), lambda i: (i, 0)),
            pl.BlockSpec((SPAN, width), lambda i: (i, 0)),
            pl.BlockSpec((SPAN, LANES), lambda i: (i, 0)),
            fixed((inner, width)),
            pl.BlockSpec((SPAN, inner), lambda i: (i, 0)),
            fixed((1, inner)),
            fixed((LANES, inner)),
        ],
        out_specs=[
            pl.BlockSpec((SPAN, inner), lambda i: (i, 0)),
            pl.BlockSpec((SPAN, inner), lambda i: (i, 0)),
            pl.BlockSpec((8, SPAN), lambda i: (0, i)),
        ],
        out_shape=[
            jax.ShapeDtypeStruct((rows, inner), f32),
            jax.ShapeDtypeStruct((rows, inner), bf16),
            jax.ShapeDtypeStruct((8, rows), f32),
        ],
        compiler_params=params(),
        cost_estimate=cost(rows * inner * width * 4, rows * inner * 14, rows * inner),
        name="gate_forward",
    )(y_zero, state_c, opened, entering, zx, gain, wide)


def gate_backward(back_gated, ssd_out, zx, coefficients, gain, state_c, opened, wide):
    rows, inner = ssd_out.shape
    width = state_c.shape[1]
    return pl.pallas_call(
        gate_backward_kernel,
        grid=(rows // SPAN,),
        in_specs=[
            pl.BlockSpec((SPAN, inner), lambda i: (i, 0)),
            pl.BlockSpec((SPAN, inner), lambda i: (i, 0)),
            pl.BlockSpec((SPAN, inner), lambda i: (i, 0)),
            pl.BlockSpec((SPAN, 8), lambda i: (i, 0)),
            fixed((1, inner)),
            pl.BlockSpec((SPAN, width), lambda i: (i, 0)),
            pl.BlockSpec((SPAN, LANES), lambda i: (i, 0)),
            fixed((LANES, inner)),
        ],
        out_specs=[
            pl.BlockSpec((SPAN, inner), lambda i: (i, 0)),
            pl.BlockSpec((SPAN, inner), lambda i: (i, 0)),
            pl.BlockSpec((SPAN, inner), lambda i: (i, 0)),
            fixed((1, inner)),
            fixed((inner, width)),
        ],
        out_shape=[
            jax.ShapeDtypeStruct((rows, inner), bf16),
            jax.ShapeDtypeStruct((rows, inner), bf16),
            jax.ShapeDtypeStruct((rows, inner), bf16),
            jax.ShapeDtypeStruct((1, inner), f32),
            jax.ShapeDtypeStruct((inner, width), f32),
        ],
        compiler_params=params(),
        cost_estimate=cost(rows * inner * width * 4, rows * inner * 18, rows * inner),
        name="gate_backward",
    )(back_gated, ssd_out, zx, coefficients, gain, state_c, opened, wide)


def attention(low_blocks, query_array, back_attended, pieces, segc, segr, att_pad, rows):
    pairs = att_pad // LANES
    scale = 1.0 / math.sqrt(ATT_DIM)
    count = len(pieces)

    def lane(offset):
        return pl.BlockSpec((rows, LANES), lambda p, *unused: (0, p + offset))

    in_specs = [lane(0), lane(0)]
    operands = [query_array, back_attended]
    for array, offset in pieces:
        in_specs += [lane(offset), lane(offset + pairs)]
        operands += [array, array]
    in_specs += [fixed((count * rows, 1)), fixed((1, rows))]
    shapes = [bf16, f32] + [f32, f32] + [bf16, bf16] * (count - 1)
    return pl.pallas_call(
        partial(attention_kernel, scale=scale),
        grid_spec=pltpu.PrefetchScalarGridSpec(
            num_scalar_prefetch=1,
            grid=(pairs,),
            in_specs=in_specs,
            out_specs=[lane(0)] * len(shapes),
            scratch_shapes=[
                pltpu.VMEM((count * rows, LANES), f32),
                pltpu.VMEM((count * rows, LANES), f32),
                pltpu.VMEM((LANES, SPAN), f32),
                pltpu.VMEM((8, SPAN), f32),
                pltpu.VMEM((LANES, SPAN), f32),
            ],
        ),
        out_shape=[jax.ShapeDtypeStruct((rows, att_pad), kind) for kind in shapes],
        compiler_params=params(),
        cost_estimate=cost(rows * rows * att_pad * 28, rows * att_pad * 30, rows * rows * pairs * 4),
        name="attention",
    )(low_blocks, *operands, segc, segr)


def fit(value, size, axis):
    if value.shape[axis] == size:
        return value
    widths = [(0, 0)] * value.ndim
    widths[axis] = (0, size - value.shape[axis])
    return jnp.pad(value, widths)


def head_gather(values):
    return lax.all_gather(values, "head", axis=1, tiled=True)


def head_scatter(values):
    return lax.psum_scatter(values, "head", scatter_dimension=1, tiled=True)


def seq_scatter(values):
    return lax.psum_scatter(values.astype(bf16), "seq", scatter_dimension=0, tiled=True).astype(f32)


def matmul(a, b, kind=f32):
    return jnp.dot(a, b, preferred_element_type=f32).astype(kind)


def matmul_nt(a, b, kind=f32):
    return lax.dot_general(a, b, (((1,), (1,)), ((), ())), preferred_element_type=f32).astype(kind)


def matmul_tn(a, b, kind=f32):
    return lax.dot_general(a, b, (((0,), (0,)), ((), ())), preferred_element_type=f32).astype(kind)


MESH = pl.DeviceIdType.MESH


class HeadPlace:
    def __init__(self, count):
        self.count = count
        self.chips = count // 2
        self.me = lax.axis_index("head")
        self.core = lax.rem(self.me, 2)
        self.chip = self.me // 2
        self.partner = self.chip * 2 + (1 - self.core)

    def ahead(self, step):
        return lax.rem(self.chip + step, self.chips) * 2 + self.core

    def behind(self, step):
        return lax.rem(self.chip + self.chips - step, self.chips) * 2 + self.core

    def meet(self):
        barrier = pltpu.get_barrier_semaphore()
        others = [self.partner] + [self.ahead(step) for step in range(1, self.chips)]
        for other in others:
            pl.semaphore_signal(barrier, inc=1, device_id={"head": other}, device_id_type=MESH)
        pl.semaphore_wait(barrier, len(others))


def remote(source, target, send, receive, device):
    return pltpu.make_async_remote_copy(
        src_ref=source, dst_ref=target, send_sem=send, recv_sem=receive,
        device_id={"head": device}, device_id_type=MESH,
    )


class TwoLevelGather:
    def __init__(self, place, own_at, full_at, send, receive, parts):
        self.place, self.own_at, self.full_at = place, own_at, full_at
        self.send, self.receive, self.parts = send, receive, parts

    def copy(self, kind, part):
        place = self.place
        slot = kind * self.parts + part
        send, receive = self.send.at[slot], self.receive.at[slot]
        if kind == 0:
            return remote(self.own_at(part), self.full_at(place.me, part), send, receive, place.partner)
        if kind < place.chips:
            return remote(self.own_at(part), self.full_at(place.me, part), send, receive, place.ahead(kind))
        origin = place.behind(kind - place.chips + 1)
        return remote(self.full_at(origin, part), self.full_at(origin, part), send, receive, place.partner)

    def kinds(self):
        return 2 * self.place.chips - 1

    def start(self, part):
        for kind in list(range(1, self.place.chips)) + [0]:
            self.copy(kind, part).start()

    def arrive(self, part):
        for step in range(1, self.place.chips):
            self.copy(step, part).wait_recv()
            self.copy(self.place.chips + step - 1, part).start()
        self.copy(0, part).wait_recv()
        for step in range(1, self.place.chips):
            self.copy(self.place.chips + step - 1, part).wait_recv()

    def finish(self, part):
        for kind in range(self.kinds()):
            self.copy(kind, part).wait_send()


class ScalarSum:
    def __init__(self, place, own, near, pair, far, send, receive):
        self.place, self.own, self.near, self.pair, self.far = place, own, near, pair, far
        self.send, self.receive = send, receive

    def first(self):
        return remote(self.own, self.near, self.send.at[0], self.receive.at[0], self.place.partner)

    def second(self, step):
        return remote(
            self.pair, self.far.at[step - 1], self.send.at[step], self.receive.at[step], self.place.ahead(step)
        )

    def start(self):
        self.first().start()

    def middle(self):
        self.first().wait_recv()
        self.pair[...] = self.own[...] + self.near[...]
        for step in range(1, self.place.chips):
            self.second(step).start()

    def total(self):
        total = self.pair[...]
        for step in range(1, self.place.chips):
            self.second(step).wait_recv()
            total = total + self.far[step - 1]
        return total

    def finish(self):
        self.first().wait_send()
        for step in range(1, self.place.chips):
            self.second(step).wait_send()


def column_of(line):
    rows = line.shape[1]
    pick = (lax.broadcasted_iota(jnp.int32, (8, LANES), 0) == 0).astype(f32)
    return dot_tn(jnp.broadcast_to(line, (8, rows)), pick, highest)


def gather_sems(chips, parts):
    slots = (2 * chips - 1) * parts
    return [pltpu.SemaphoreType.DMA((slots,)), pltpu.SemaphoreType.DMA((slots,))]


def scalar_scratch(chips, dense):
    return [
        pltpu.VMEM((dense, LANES), f32),
        pltpu.VMEM((dense, LANES), f32),
        pltpu.VMEM((max(chips - 1, 1), dense, LANES), f32),
        pltpu.SemaphoreType.DMA((chips,)),
        pltpu.SemaphoreType.DMA((chips,)),
    ]


def comm_params(ident):
    return pltpu.CompilerParams(vmem_limit_bytes=VMEM_LIMIT, collective_id=ident, has_side_effects=True)


VMEM = pl.BlockSpec(memory_space=pltpu.VMEM)
CHUNK = 256


def first_gather_kernel(
    count, products, tokens_ref, gain_ref, *refs
):
    weights, (full_ref, rms_ref), outs = refs[:products], refs[products : products + 2], refs[products + 2 : 2 * products + 2]
    raw, gains, send, receive, gsend, greceive = refs[2 * products + 2 :]
    rows, features = tokens_ref.shape
    place = HeadPlace(count)
    parts = rows // CHUNK

    def rows_of(part):
        return pl.ds(pl.multiple_of(part * CHUNK, CHUNK), CHUNK)

    data = TwoLevelGather(
        place, lambda part: tokens_ref.at[rows_of(part)], lambda who, part: raw.at[who, rows_of(part)],
        send, receive, parts,
    )
    gain = TwoLevelGather(place, lambda part: gain_ref, lambda who, part: gains.at[who], gsend, greceive, 1)
    place.meet()
    gain.start(0)
    lax.fori_loop(0, parts, lambda part, unused: (data.start(part), unused)[1], 0)
    gains[place.me] = gain_ref[...]
    raw[place.me] = tokens_ref[...]
    gain.arrive(0)

    def step(part, unused):
        data.arrive(part)
        where = rows_of(part)
        values = [raw[who, where, :].astype(f32) for who in range(count)]
        total = sum(jnp.sum(value * value, axis=1, keepdims=True) for value in values)
        scale = lax.rsqrt(total / (count * features) + epsilon)
        rms_ref[where, :] = jnp.broadcast_to(scale, (CHUNK, 8))
        sums = [jnp.zeros((CHUNK, out.shape[1]), f32) for out in outs]
        for who in range(count):
            normed = (values[who] * scale * gains[who, 0:1, :]).astype(bf16)
            full_ref[who, where, :] = normed
            inner_rows = slice(who * features, (who + 1) * features)
            sums = [value + dot_nn(normed, weight[inner_rows, :]) for value, weight in zip(sums, weights)]
        for out, value in zip(outs, sums):
            out[where, :] = value
        return unused

    lax.fori_loop(0, parts, step, 0)
    gain.finish(0)
    lax.fori_loop(0, parts, lambda part, unused: (data.finish(part), unused)[1], 0)


def first_gather(tokens, gain, weights, ident):
    rows, features = tokens.shape
    count = D // features
    chips = count // 2
    return pl.pallas_call(
        partial(first_gather_kernel, count, len(weights)),
        in_specs=[VMEM] * (2 + len(weights)),
        out_specs=[VMEM] * (2 + len(weights)),
        out_shape=[
            jax.ShapeDtypeStruct((count, rows, features), bf16),
            jax.ShapeDtypeStruct((rows, 8), f32),
        ]
        + [jax.ShapeDtypeStruct((rows, weight.shape[1]), f32) for weight in weights],
        scratch_shapes=[
            pltpu.VMEM((count, rows, features), bf16),
            pltpu.VMEM((count, 8, features), f32),
        ]
        + gather_sems(chips, rows // CHUNK)
        + gather_sems(chips, 1),
        compiler_params=comm_params(ident),
        cost_estimate=cost(2 * rows * D * sum(weight.shape[1] for weight in weights), 30e6),
        name="first_gather",
    )(tokens, fit(gain[None], 8, 0), *weights)


def gather_kernel(
    count, transposed, scaled, own_ref, dense_ref, weight_ref,
    full_ref, total_ref, out_ref,
    send, receive, near, pair, far, ssend, sreceive,
):
    rows, features = own_ref.shape
    place = HeadPlace(count)
    parts = rows // CHUNK

    def rows_of(part):
        return pl.ds(pl.multiple_of(part * CHUNK, CHUNK), CHUNK)

    data = TwoLevelGather(
        place, lambda part: own_ref.at[rows_of(part)], lambda who, part: full_ref.at[who, rows_of(part)],
        send, receive, parts,
    )
    scalars = ScalarSum(place, dense_ref, near, pair, far, ssend, sreceive)
    place.meet()
    scalars.start()
    lax.fori_loop(0, parts, lambda part, unused: (data.start(part), unused)[1], 0)
    scalars.middle()
    full_ref[place.me] = own_ref[...]
    total = scalars.total()
    total_ref[...] = total
    if scaled:
        near[...] = lax.rsqrt(total / (count * features) + epsilon)

    def step(part, unused):
        data.arrive(part)
        where = rows_of(part)
        out = jnp.zeros((CHUNK, out_ref.shape[1]), f32)
        for who in range(count):
            piece = full_ref[who, where, :]
            if transposed:
                out = out + dot_nt(piece, weight_ref[:, who * features : (who + 1) * features])
            else:
                out = out + dot_nn(piece, weight_ref[who * features : (who + 1) * features, :])
        if scaled:
            per = CHUNK // LANES
            line = jnp.concatenate([near[pl.ds(part * per + i, 1), :] for i in range(per)], axis=1)
            out = out * column_of(line)[:, 0:1]
        out_ref[where, :] = out.astype(out_ref.dtype)
        return unused

    lax.fori_loop(0, parts, step, 0)
    scalars.finish()
    lax.fori_loop(0, parts, lambda part, unused: (data.finish(part), unused)[1], 0)


def gather_matmul(own, sums, weight, transposed, scaled, ident, name):
    rows, features = own.shape
    count = D // features
    chips = count // 2
    columns = weight.shape[0 if transposed else 1]
    dense = rows // LANES
    return pl.pallas_call(
        partial(gather_kernel, count, transposed, scaled),
        in_specs=[VMEM] * 3,
        out_specs=[VMEM] * 3,
        out_shape=[
            jax.ShapeDtypeStruct((count, rows, features), bf16),
            jax.ShapeDtypeStruct((dense, LANES), f32),
            jax.ShapeDtypeStruct((rows, columns), bf16),
        ],
        scratch_shapes=gather_sems(chips, rows // CHUNK) + scalar_scratch(chips, dense),
        compiler_params=comm_params(ident),
        cost_estimate=cost(2 * rows * D * columns, 20e6),
        name=name,
    )(own, sums.reshape(dense, LANES), weight)


def scatter_kernel(count, operands, transposed, *refs):
    lefts, rights = refs[:operands], refs[operands : 2 * operands]
    dense_ref, out_ref, total_ref = refs[2 * operands : 2 * operands + 3]
    (own, near_data, sent, far_data, psend, preceive, xsend, xreceive,
     near, pair, far, ssend, sreceive) = refs[2 * operands + 3 :]
    rows, features = out_ref.shape
    place = HeadPlace(count)
    chips = place.chips
    parts = rows // CHUNK

    def rows_of(part):
        return pl.ds(pl.multiple_of(part * CHUNK, CHUNK), CHUNK)

    def to_partner(chip, part):
        slot = chip * parts + part
        return remote(
            own.at[chip * 2 + 1 - place.core, rows_of(part)], near_data.at[chip, rows_of(part)],
            psend.at[slot], preceive.at[slot], place.partner,
        )

    def across(step, part):
        slot = (step - 1) * parts + part
        return remote(
            sent.at[step - 1, rows_of(part)], far_data.at[step - 1, rows_of(part)],
            xsend.at[slot], xreceive.at[slot], place.ahead(step),
        )

    scalars = ScalarSum(place, dense_ref, near, pair, far, ssend, sreceive)
    place.meet()
    scalars.start()

    def compute(part):
        where = rows_of(part)
        for who in range(count):
            inner = slice(who * features, (who + 1) * features)
            value = jnp.zeros((CHUNK, features), f32)
            for left, right in zip(lefts, rights):
                if transposed:
                    value = value + dot_nt(left[where, :], right[inner, :])
                else:
                    value = value + dot_nn(left[where, :], right[:, inner])
            own[who, where, :] = value.astype(bf16)
        for chip in range(chips):
            to_partner(chip, part).start()

    def combine(part):
        where = rows_of(part)
        for chip in range(chips):
            to_partner(chip, part).wait_recv()
        for step in range(1, chips):
            chip = lax.rem(place.chip + step, chips)
            mine = own[chip * 2 + place.core, where, :].astype(f32)
            sent[step - 1, where, :] = (mine + near_data[chip, where, :].astype(f32)).astype(bf16)
            across(step, part).start()

    compute(0)
    scalars.middle()

    def forward(part, unused):
        compute(part)
        combine(part - 1)
        return unused

    lax.fori_loop(1, parts, forward, 0)
    combine(parts - 1)
    total_ref[...] = scalars.total()

    def collect(part, unused):
        where = rows_of(part)
        value = own[place.me, where, :].astype(f32) + near_data[place.chip, where, :].astype(f32)
        for step in range(1, chips):
            across(step, part).wait_recv()
            value = value + far_data[step - 1, where, :].astype(f32)
        out_ref[where, :] = value
        return unused

    lax.fori_loop(0, parts, collect, 0)
    scalars.finish()

    def drain(part, unused):
        for chip in range(chips):
            to_partner(chip, part).wait_send()
        for step in range(1, chips):
            across(step, part).wait_send()
        return unused

    lax.fori_loop(0, parts, drain, 0)


def matmul_scatter(lefts, rights, sums, transposed, count, ident, name):
    rows = lefts[0].shape[0]
    features = D // count
    chips = count // 2
    dense = rows // LANES
    parts = rows // CHUNK
    flops = sum(2 * rows * D * left.shape[1] for left in lefts)
    return pl.pallas_call(
        partial(scatter_kernel, count, len(lefts), transposed),
        in_specs=[VMEM] * (2 * len(lefts) + 1),
        out_specs=[VMEM] * 2,
        out_shape=[
            jax.ShapeDtypeStruct((rows, features), f32),
            jax.ShapeDtypeStruct((dense, LANES), f32),
        ],
        scratch_shapes=[
            pltpu.VMEM((count, rows, features), bf16),
            pltpu.VMEM((chips, rows, features), bf16),
            pltpu.VMEM((max(chips - 1, 1), rows, features), bf16),
            pltpu.VMEM((max(chips - 1, 1), rows, features), bf16),
            pltpu.SemaphoreType.DMA((chips * parts,)),
            pltpu.SemaphoreType.DMA((chips * parts,)),
            pltpu.SemaphoreType.DMA((max(chips - 1, 1) * parts,)),
            pltpu.SemaphoreType.DMA((max(chips - 1, 1) * parts,)),
        ]
        + scalar_scratch(chips, dense),
        compiler_params=comm_params(ident),
        cost_estimate=cost(flops, 20e6),
        name=name,
    )(*lefts, *rights, sums.reshape(dense, LANES))


def weight_grad_kernel(products, left_ref, *refs):
    left = left_ref[...]
    for right, out in zip(refs[:products], refs[products:]):
        out[...] = dot_tn(left, right[...]).astype(out.dtype)


def weight_grad(full, rights, name):
    count, rows, features = full.shape
    columns = [right.shape[1] for right in rights]
    return pl.pallas_call(
        partial(weight_grad_kernel, len(rights)),
        grid=(count,),
        in_specs=[pl.BlockSpec((None, rows, features), lambda i: (i, 0, 0))] + [fixed((rows, n)) for n in columns],
        out_specs=[pl.BlockSpec((features, n), lambda i: (i, 0)) for n in columns],
        out_shape=[jax.ShapeDtypeStruct((count * features, n), bf16) for n in columns],
        compiler_params=params(),
        cost_estimate=cost(2 * rows * D * sum(columns), 2 * (rows + D) * (D + sum(columns))),
        name=name,
    )(full, *rights)


def gathered_product_kernel(full_ref, weight_ref, out_ref):
    count, rows, features = full_ref.shape
    value = jnp.zeros(out_ref.shape, f32)
    for who in range(count):
        value = value + dot_nt(full_ref[who], weight_ref[:, who * features : (who + 1) * features])
    out_ref[...] = value.astype(out_ref.dtype)


def gathered_product(full, weight, name):
    count, rows, features = full.shape
    columns = weight.shape[0]
    return pl.pallas_call(
        gathered_product_kernel,
        grid=(rows // CHUNK,),
        in_specs=[pl.BlockSpec((count, CHUNK, features), lambda i: (0, i, 0)), fixed(weight.shape)],
        out_specs=pl.BlockSpec((CHUNK, columns), lambda i: (i, 0)),
        out_shape=jax.ShapeDtypeStruct((rows, columns), bf16),
        compiler_params=params(),
        cost_estimate=cost(2 * rows * D * columns, 2 * (rows * D + D * columns + rows * columns)),
        name=name,
    )(full, weight)


def spread_product_kernel(left_ref, weight_ref, out_ref):
    features = out_ref.shape[2]
    for who in range(out_ref.shape[0]):
        out_ref[who] = dot_nn(left_ref[...], weight_ref[:, who * features : (who + 1) * features]).astype(out_ref.dtype)


def spread_product(left, weight, count, name):
    rows, depth = left.shape
    features = weight.shape[1] // count
    return pl.pallas_call(
        spread_product_kernel,
        grid=(rows // CHUNK,),
        in_specs=[pl.BlockSpec((CHUNK, depth), lambda i: (i, 0)), fixed(weight.shape)],
        out_specs=pl.BlockSpec((count, CHUNK, features), lambda i: (0, i, 0)),
        out_shape=jax.ShapeDtypeStruct((count, rows, features), bf16),
        compiler_params=params(),
        cost_estimate=cost(2 * rows * D * depth, 2 * (rows * D + D * depth + rows * depth)),
        name=name,
    )(left, weight)


def per_device(
    tokens, segment_ids, first_gain, proj_zx, proj_bc, proj_step, conv_inner, conv_inner_bias,
    conv_state, conv_state_bias, step_bias, decay_log, skip_scale, gated_gain, proj_out,
    second_gain, proj_qkv, attention_out, cotangent,
):
    rows = tokens.shape[0]
    inner = proj_zx.shape[2]
    bc_width = proj_bc.shape[1]
    width = bc_width // 2
    channels = inner + bc_width
    heads = step_bias.shape[0]
    att = proj_qkv.shape[2]
    att_pad = -(-att // LANES) * LANES
    pairs = att_pad // LANES
    blocks = rows // SPAN
    reach = (DOC_MAX - 2) // rows + 1
    row_start = lax.axis_index("seq") * rows

    padded_seg = jnp.concatenate([jnp.full((reach * rows,), -1, jnp.int32), segment_ids])
    window = lax.dynamic_slice_in_dim(padded_seg, row_start, (reach + 1) * rows)
    local_seg = window[reach * rows :]
    shifted = window[reach * rows - (CONV - 1) :]
    kept = jnp.stack([(shifted[tap : tap + rows] == local_seg).astype(f32) for tap in range(CONV - 1)], axis=1)
    kept = fit(kept, 8, 1)
    span_prev = shifted[CONV - 2 :: SPAN][:blocks]
    span_last = local_seg[SPAN - 1 :: SPAN]
    segc_window = window[:, None]
    segc = local_seg[:, None]
    segr = local_seg[None, :]
    key_last = window[SPAN - 1 :: SPAN].reshape(reach + 1, blocks)
    query_first = local_seg[::SPAN]
    low_blocks = jnp.sum((key_last[None] < query_first[:, None, None]).astype(jnp.int32), axis=2).reshape(-1)

    owner = jnp.arange(inner, dtype=jnp.int32)[None, :] // SSM_DIM
    wide = (owner == jnp.arange(LANES, dtype=jnp.int32)[:, None]).astype(f32)
    tall = wide.T
    constants = (
        jnp.concatenate([conv_inner, conv_state], axis=1),
        jnp.concatenate([conv_inner_bias, conv_state_bias])[None],
        fit(step_bias[None], LANES, 1),
        fit(-jnp.exp(decay_log)[None], LANES, 1),
        jnp.repeat(skip_scale, SSM_DIM)[None],
        wide,
        tall,
    )
    count = lax.axis_size("head")
    gate_weight, inner_weight = proj_zx[:, 0, :], proj_zx[:, 1, :]
    bcs_weight = jnp.concatenate([proj_bc, fit(proj_step, LANES, 1)], axis=1)
    qkv_weight = fit(proj_qkv, att_pad, 2).reshape(D, 3 * att_pad)
    att_weight = fit(attention_out, att_pad, 0)

    first_full, first_rms, zed, inner_x, bcs = first_gather(
        tokens, first_gain, (gate_weight, inner_weight, bcs_weight), 0
    )
    first_rms = first_rms[:, 0:1]
    cot_full = lax.all_gather(cotangent, "head")
    edge_rows = jnp.concatenate([inner_x[rows - 8 :], bcs[rows - 8 :, :bc_width]], axis=1)
    edge = from_behind(edge_rows, "seq", 1)

    ssd_shared = (span_prev, span_last, inner_x, bcs, edge, kept, segc, segr)
    y_zero, state_c, opened, states, end_state, through = ssd_forward(*ssd_shared, constants, inner, width)

    sent = end_state.astype(bf16)
    packed = jnp.concatenate([sent, jnp.broadcast_to(through[0:1], (8, LANES)).astype(bf16)], axis=0)
    near_pack = from_behind(packed, "seq", 1).astype(f32)
    near_through = jnp.repeat(near_pack[inner, :heads], SSM_DIM)[:, None]
    far = from_behind(sent, "seq", 2).astype(f32)
    entering = (near_pack[:inner] + near_through * far).astype(bf16)

    ssd_out, gated_raw, gate_sums = gate_forward(y_zero, state_c, opened, entering, zed, gated_gain[None], wide)
    branch_raw, gate_total = matmul_scatter(
        (gated_raw,), (proj_out,), gate_sums[0], False, count, 1, "branch_scatter"
    )
    gate_rms = lax.rsqrt(gate_total.reshape(rows, 1) / INNER + epsilon)
    branch = branch_raw * gate_rms
    hidden_zero = tokens.astype(f32)
    hidden_one = hidden_zero + branch
    second_full, second_total, projected = gather_matmul(
        (hidden_one * second_gain).astype(bf16), jnp.sum(hidden_one * hidden_one, axis=1),
        qkv_weight, False, True, 2, "second_gather",
    )
    second_rms = lax.rsqrt(second_total.reshape(rows, 1) / D + epsilon)
    key_value = projected[:, att_pad:]
    moved = [from_behind(key_value, "seq", back) for back in range(1, reach + 1)]

    back_attended = gathered_product(cot_full, att_weight, "back_attended")
    pieces = [(projected, pairs)] + [(array, 0) for array in moved]
    attended, back_query, back_key, back_value, *back_moved = attention(
        low_blocks, projected, back_attended, pieces, segc_window, segr, att_pad, rows
    )
    out_part = spread_product(attended, att_weight, count, "output_product")
    output = (
        hidden_one + lax.psum_scatter(out_part, "head", scatter_dimension=0).astype(f32)
    ).astype(bf16)
    (grad_att,) = weight_grad(cot_full, (attended,), "grad_attention_out")

    for back in range(1, reach + 1):
        pair = jnp.concatenate(back_moved[2 * back - 2 : 2 * back], axis=1)
        pair = from_behind(pair, "seq", -back).astype(f32)
        back_key = back_key + pair[:, :att_pad]
        back_value = back_value + pair[:, att_pad:]
    back_projected = jnp.concatenate([back_query, back_key, back_value], axis=1).astype(bf16)
    second_sums = jnp.sum(back_projected.astype(f32) * projected.astype(f32), axis=1)
    back_second, second_dots = matmul_scatter(
        (back_projected,), (qkv_weight,), second_sums, True, count, 3, "second_scatter"
    )
    (grad_qkv,) = weight_grad(
        second_full, ((back_projected.astype(f32) * second_rms).astype(bf16),), "grad_qkv"
    )
    if att != att_pad:
        grad_att = grad_att[:, :att]
        grad_qkv = grad_qkv.reshape(D, 3, att_pad)[:, :, :att].reshape(D, 3 * att)
    grad_second_gain = jnp.sum(hidden_one * second_rms * back_second, axis=0)
    back_hidden_one = (
        cotangent.astype(f32)
        + second_rms * second_gain * back_second
        - hidden_one * (second_rms * second_rms / D * second_dots.reshape(rows, 1))
    )
    back_low = back_hidden_one.astype(bf16)
    back_branch, gate_dots, back_gated = gather_matmul(
        back_low, jnp.sum(back_low.astype(f32) * branch, axis=1), proj_out, True, False, 4, "branch_gather"
    )
    coefficients = fit(
        jnp.concatenate([gate_rms, gate_rms * gate_rms / INNER * gate_dots.reshape(rows, 1)], axis=1), 8, 1
    )
    dy, back_z, gated, grad_gated_gain, back_entering = gate_backward(
        back_gated, ssd_out, zed, coefficients, gated_gain[None], state_c, opened, wide
    )

    back_sent = back_entering.astype(bf16)
    back_pack = jnp.concatenate([back_sent, jnp.broadcast_to(through[0:1], (8, LANES)).astype(bf16)], axis=0)
    back_near_pack = from_behind(back_pack, "seq", -1).astype(f32)
    back_far = from_behind(back_sent, "seq", -2).astype(f32)
    back_near_through = jnp.repeat(back_near_pack[inner, :heads], SSM_DIM)[:, None]
    back_end = back_near_pack[:inner] + back_near_through * back_far
    (grad_out,) = weight_grad(back_branch, (gated,), "grad_out")
    (grad_gate,) = weight_grad(first_full, (back_z,), "grad_gate")

    back_x, back_bc, back_step, tail_rows, back_edge, grad_conv, grad_heads = ssd_backward(
        *ssd_shared, dy, states, opened, entering, back_end, constants, inner, width
    )
    tail_rows = (tail_rows + from_behind(back_edge, "seq", -1)).astype(bf16)
    back_x = lax.dynamic_update_slice(back_x, tail_rows[:, :inner], (rows - 8, 0))
    back_bc = lax.dynamic_update_slice(back_bc, tail_rows[:, inner:], (rows - 8, 0))
    grad_inner, grad_bc, grad_step = weight_grad(first_full, (back_x, back_bc, back_step), "grad_inner")
    first_sums = (
        jnp.sum(back_z.astype(f32) * zed, axis=1)
        + jnp.sum(back_x.astype(f32) * inner_x, axis=1)
        + jnp.sum(back_bc.astype(f32) * bcs[:, :bc_width], axis=1)
        + jnp.sum(back_step.astype(f32) * bcs[:, bc_width:], axis=1)
    )
    back_first, first_dots = matmul_scatter(
        (back_z, back_x, back_bc, back_step),
        (gate_weight, inner_weight, proj_bc, bcs_weight[:, bc_width:]),
        first_sums, True, count, 5, "first_scatter",
    )
    grad_first_gain = jnp.sum(hidden_zero * first_rms * back_first, axis=0)
    grad_tokens = (
        back_hidden_one
        + first_rms * first_gain * back_first
        - hidden_zero * (first_rms * first_rms / D * first_dots.reshape(rows, 1))
    ).astype(bf16)

    wide_att = seq_scatter(grad_att).T
    wide_qkv = seq_scatter(grad_qkv).reshape(-1, 3, att)
    wide_out = seq_scatter(grad_out).T
    wide_gate = seq_scatter(grad_gate)
    wide_tail = seq_scatter(jnp.concatenate([grad_inner, grad_step], axis=1))
    wide_zx = jnp.stack([wide_gate, wide_tail[:, :inner]], axis=1)
    wide_step = wide_tail[:, inner : inner + heads]
    shared_bc = lax.psum_scatter(grad_bc, ("seq", "head"), scatter_dimension=1, tiled=True).astype(f32)
    small = lax.psum(
        (
            grad_first_gain,
            grad_conv[:5],
            grad_heads[:3, :heads],
            grad_gated_gain[0],
            grad_second_gain,
        ),
        "seq",
    )
    shared = bc_width // (lax.axis_size("seq") * count)
    shared_at = (lax.axis_index("seq") * count + lax.axis_index("head")) * shared
    shared_conv = lax.dynamic_slice_in_dim(lax.psum(small[1][:, inner:], "head"), shared_at, shared, 1)
    return (
        output,
        grad_tokens,
        small[0],
        wide_zx,
        shared_bc,
        wide_step,
        small[1][:4, :inner],
        small[1][4, :inner],
        shared_conv[:4],
        shared_conv[4],
        small[2][0],
        small[2][1],
        small[2][2],
        small[3],
        wide_out,
        small[4],
        wide_qkv,
        wide_att,
    )


def solution(mesh):
    placed = (
        P("seq", "head"),
        P(),
        P("head"),
        P(None, None, "head"),
        P(),
        P(None, "head"),
        P(None, "head"),
        P("head"),
        P(),
        P(),
        P("head"),
        P("head"),
        P("head"),
        P("head"),
        P("head", None),
        P("head"),
        P(None, None, "head"),
        P("head", None),
        P("seq", "head"),
    )
    return jax.shard_map(
        per_device,
        mesh=mesh,
        in_specs=placed,
        out_specs=(
            P("seq", "head"),
            P("seq", "head"),
            P("head"),
            P("seq", None, "head"),
            P(None, ("seq", "head")),
            P("seq", "head"),
            P(None, "head"),
            P("head"),
            P(None, ("seq", "head")),
            P(("seq", "head")),
            P("head"),
            P("head"),
            P("head"),
            P("head"),
            P("head", "seq"),
            P("head"),
            P("seq", None, "head"),
            P("head", "seq"),
        ),
        check_vma=False,
    )
```

```python
from functools import partial
import math

import jax
import jax.numpy as jnp
from jax import lax
from jax.experimental import pallas as pl
from jax.experimental.pallas import tpu as pltpu
from jax.sharding import PartitionSpec as P

D = 1536
ATT_DIM = 64
SSM_DIM = 64
SPAN = 256
CONV = 4
DOC_MAX = 2000
INNER = 3072
LANES = 128

epsilon = 1e-05
highest = lax.Precision.HIGHEST
f32 = jnp.float32
bf16 = jnp.bfloat16
masked_score = -1e30
VMEM_LIMIT = 60 * 1024 * 1024


def dot_nn(a, b, precision=None):
    return lax.dot_general(a, b, (((1,), (0,)), ((), ())), precision=precision, preferred_element_type=f32)


def dot_nt(a, b, precision=None):
    return lax.dot_general(a, b, (((1,), (1,)), ((), ())), precision=precision, preferred_element_type=f32)


def dot_tn(a, b, precision=None):
    return lax.dot_general(a, b, (((0,), (0,)), ((), ())), precision=precision, preferred_element_type=f32)


def softplus(x):
    return jnp.maximum(x, 0.0) + jnp.log1p(jnp.exp(-jnp.abs(x)))


def sigmoid(x):
    return 1.0 / (1.0 + jnp.exp(-x))


def lane_low(rows):
    return lax.broadcasted_iota(jnp.int32, (rows, LANES), 1) < SSM_DIM


def conv_rows(buf, weight, bias, kept, rows):
    summed = bias + weight[3:4, :] * buf[8 : 8 + rows, :]
    for tap in range(3):
        summed = summed + weight[tap : tap + 1, :] * (buf[5 + tap : 5 + tap + rows, :] * kept[:, tap : tap + 1])
    return summed


def fill_conv(buf, chunk, x_ref, xprev_ref, bcs_ref, bprev_ref, edge_ref, inner, rows):
    buf[8 : 8 + rows, :inner] = x_ref[...]
    buf[8 : 8 + rows, inner:] = bcs_ref[:, : buf.shape[1] - inner]

    @pl.when(chunk == 0)
    def _():
        buf[0:8, :] = edge_ref[...]

    @pl.when(chunk > 0)
    def _():
        buf[0:8, :inner] = xprev_ref[...]
        buf[0:8, inner:] = bprev_ref[:, : buf.shape[1] - inner]


def span_terms(bcs_ref, bc_width, bias_ref, rate_ref, segc_ref, segr_ref, prev, last, rows):
    raw = bcs_ref[:, bc_width:] + bias_ref[...]
    step = softplus(raw)
    decay = rate_ref[...] * step
    row = lax.broadcasted_iota(jnp.int32, (rows, rows), 0)
    col = lax.broadcasted_iota(jnp.int32, (rows, rows), 1)
    causal = row >= col
    tri = causal.astype(f32)
    cum = dot_nn(tri, decay, highest)
    segc = segc_ref[...]
    allowed = (segc == segr_ref[...]) & causal
    opened = (segc == prev).astype(f32)
    closing = (segc == last).astype(f32)
    last_cum = cum[rows - 1 : rows, :]
    enter = jnp.exp(cum) * opened
    tail = jnp.exp(last_cum - cum) * closing
    through = jnp.exp(last_cum) * (last == prev).astype(f32)
    return raw, step, decay, cum, tri, allowed, enter, tail, last_cum, through


def ssd_forward_kernel(
    prev_ref, last_ref, x_ref, xprev_ref, bcs_ref, bprev_ref, edge_ref, kept_ref, segc_ref, segr_ref,
    weight_ref, cbias_ref, bias_ref, rate_ref, skip_ref, wide_ref, tall_ref,
    y_ref, c_ref, open_ref, states_ref, end_ref, through_ref,
    state, base, buf,
):
    chunk = pl.program_id(0)
    rows = x_ref.shape[0]
    inner = x_ref.shape[1]
    width = c_ref.shape[1]
    heads = inner // SSM_DIM

    @pl.when(chunk == 0)
    def _():
        state[...] = jnp.zeros_like(state)
        base[...] = jnp.zeros_like(base)

    fill_conv(buf, chunk, x_ref, xprev_ref, bcs_ref, bprev_ref, edge_ref, inner, rows)
    pre = conv_rows(buf, weight_ref[...], cbias_ref[...], kept_ref[...], rows)
    conv = pre * sigmoid(pre)
    values = conv[:, :inner]
    b_low = conv[:, inner : inner + width].astype(bf16)
    c_low = conv[:, inner + width :].astype(bf16)
    prev, last, prev_dev = prev_ref[chunk], last_ref[chunk], prev_ref[0]
    raw, step, decay, cum, tri, allowed, enter, tail, last_cum, through = span_terms(
        bcs_ref, 2 * width, bias_ref, rate_ref, segc_ref, segr_ref, prev, last, rows
    )
    cum_t = cum.T
    inter = jnp.where(allowed, dot_nt(c_low, b_low), 0.0)
    wide = wide_ref[...]
    scaled = values * dot_nn(step, wide, highest)
    scaled_low = scaled.astype(bf16)
    old = state[...]
    old_low = old.astype(bf16)
    states_ref[...] = old_low
    c_ref[...] = c_low
    carried = dot_nt(c_low, old_low) * dot_nn(enter, wide, highest) + skip_ref[...] * values
    low = lane_low(rows)
    for pair in range(heads // 2):
        cols = slice(pair * LANES, (pair + 1) * LANES)
        both = []
        for head in (2 * pair, 2 * pair + 1):
            spread = jnp.exp(jnp.minimum(cum[:, head : head + 1] - cum_t[head : head + 1, :], 0.0))
            both.append(dot_nn((inter * spread).astype(bf16), scaled_low[:, cols]))
        y_ref[:, cols] = jnp.where(low, both[0], both[1]) + carried[:, cols]
    fresh = dot_tn((scaled * dot_nn(tail, wide, highest)).astype(bf16), b_low)
    through_rows = jnp.broadcast_to(through, (8, LANES))
    column = dot_nt(tall_ref[...], through_rows, highest)[:, 0:1]
    new = old * column + fresh
    state[...] = new
    end_ref[...] = new
    total = base[0:1, :]
    open_ref[...] = jnp.exp(total + cum) * (segc_ref[...] == prev_dev).astype(f32)
    base[...] = jnp.broadcast_to(total + last_cum, base.shape)
    through_ref[...] = jnp.broadcast_to(
        jnp.exp(total + last_cum) * (last == prev_dev).astype(f32), through_ref.shape
    )


def gate_forward_kernel(y_ref, c_ref, open_ref, enter_ref, z_ref, gain_ref, wide_ref, ssd_ref, out_ref, sum_ref):
    ssd = y_ref[...] + dot_nt(c_ref[...], enter_ref[...]) * dot_nn(open_ref[...], wide_ref[...], highest)
    z = z_ref[...]
    mixed = ssd * (z * sigmoid(z))
    ssd_ref[...] = ssd
    out_ref[...] = (mixed * gain_ref[...]).astype(bf16)
    sum_ref[...] = dot_nt(jnp.ones((8, mixed.shape[1]), f32), mixed * mixed, highest)


def gate_backward_kernel(
    bg_ref, ssd_ref, z_ref, rc_ref, gain_ref, c_ref, open_ref, wide_ref,
    dy_ref, gz_ref, gated_ref, ggain_ref, enter_ref,
):
    @pl.when(pl.program_id(0) == 0)
    def _():
        ggain_ref[...] = jnp.zeros_like(ggain_ref)
        enter_ref[...] = jnp.zeros_like(enter_ref)

    ssd = ssd_ref[...]
    z = z_ref[...]
    sig = sigmoid(z)
    gate = z * sig
    mixed = ssd * gate
    rms = rc_ref[:, 0:1]
    back = bg_ref[...].astype(f32)
    normed = mixed * rms
    gained = back * gain_ref[...]
    g_mixed = gained * rms - mixed * rc_ref[:, 1:2]
    gated_ref[...] = (normed * gain_ref[...]).astype(bf16)
    ggain_ref[...] += jnp.sum(normed * back, axis=0, keepdims=True)
    dy = (g_mixed * gate).astype(bf16)
    dy_ref[...] = dy
    gz_ref[...] = (g_mixed * ssd * (sig + gate * (1.0 - sig))).astype(bf16)
    opened = (dy.astype(f32) * dot_nn(open_ref[...], wide_ref[...], highest)).astype(bf16)
    enter_ref[...] += dot_tn(opened, c_ref[...])


def ssd_backward_kernel(
    prev_ref, last_ref, x_ref, xprev_ref, bcs_ref, bprev_ref, edge_ref, kept_ref, segc_ref, segr_ref,
    dy_ref, states_ref, openprev_ref, enter_ref, back_ref,
    weight_ref, cbias_ref, bias_ref, rate_ref, skip_ref, wide_ref, tall_ref,
    dx_ref, dbc_ref, dstep_ref, tail_ref, dedge_ref, dconv_ref, dhead_ref,
    dstate, follow, buf, grad,
):
    rows = x_ref.shape[0]
    inner = x_ref.shape[1]
    width = states_ref.shape[1]
    heads = inner // SSM_DIM
    first = pl.program_id(0) == 0
    chunk = pl.num_programs(0) - 1 - pl.program_id(0)

    @pl.when(first)
    def _():
        dstate[...] = back_ref[...]
        follow[...] = jnp.zeros_like(follow)
        dconv_ref[...] = jnp.zeros_like(dconv_ref)
        dhead_ref[...] = jnp.zeros_like(dhead_ref)

    fill_conv(buf, chunk, x_ref, xprev_ref, bcs_ref, bprev_ref, edge_ref, inner, rows)
    weight = weight_ref[...]
    kept = kept_ref[...]
    pre = conv_rows(buf, weight, cbias_ref[...], kept, rows)
    sig = sigmoid(pre)
    conv = pre * sig
    slope = sig + conv * (1.0 - sig)
    values = conv[:, :inner]
    b_low = conv[:, inner : inner + width].astype(bf16)
    c_low = conv[:, inner + width :].astype(bf16)
    prev, last = prev_ref[chunk], last_ref[chunk]
    raw, step, decay, cum, tri, allowed, enter, tail, last_cum, through = span_terms(
        bcs_ref, 2 * width, bias_ref, rate_ref, segc_ref, segr_ref, prev, last, rows
    )
    cum_t = cum.T
    inter = jnp.where(allowed, dot_nt(c_low, b_low), 0.0)
    wide = wide_ref[...]
    tall = tall_ref[...]
    step_wide = dot_nn(step, wide, highest)
    enter_wide = dot_nn(enter, wide, highest)
    tail_wide = dot_nn(tail, wide, highest)
    scaled_low = (values * step_wide).astype(bf16)
    scaled = scaled_low.astype(f32)
    dy_low = dy_ref[...]
    dy = dy_low.astype(f32)
    reach = jnp.where(chunk == 0, jnp.ones((8, LANES), f32), jnp.broadcast_to(openprev_ref[7:8, :], (8, LANES)))
    old = states_ref[...].astype(f32) + dot_nt(tall, reach, highest)[:, 0:1] * enter_ref[...].astype(f32)
    old_low = old.astype(bf16)
    dnew = dstate[...]
    dnew_low = dnew.astype(bf16)
    dy_enter = (dy * enter_wide).astype(bf16)
    from_state = dot_nt(c_low, old_low) * enter_wide
    to_state = dot_nt(b_low, dnew_low) * tail_wide
    dc = dot_nn(dy_enter, old_low)
    db = dot_nn((scaled * tail_wide).astype(bf16), dnew_low)
    through_column = dot_nt(tall, jnp.broadcast_to(through, (8, LANES)), highest)[:, 0:1]
    state_dots = jnp.sum(dnew * old, axis=1, keepdims=True) * through_column
    through_sum = jnp.sum(tall * state_dots, axis=0, keepdims=True)
    dstate[...] = dnew * through_column + dot_tn(dy_enter, c_low)
    low = lane_low(rows)
    mixed_grad = jnp.zeros((rows, rows), f32)
    within_parts = []
    dscaled_parts = []
    for pair in range(heads // 2):
        cols = slice(pair * LANES, (pair + 1) * LANES)
        scaled_pair = scaled_low[:, cols]
        dy_pair = dy_low[:, cols]
        ahead = []
        behind = []
        for index in range(2):
            head = 2 * pair + index
            spread = jnp.exp(jnp.minimum(cum[:, head : head + 1] - cum_t[head : head + 1, :], 0.0))
            mixing = (inter * spread).astype(bf16)
            dy_one = jnp.where(low if index == 0 else jnp.logical_not(low), dy_pair, jnp.zeros_like(dy_pair))
            mixed_grad = mixed_grad + dot_nt(dy_one, scaled_pair) * spread
            ahead.append(dot_nn(mixing, scaled_pair))
            behind.append(dot_tn(mixing, dy_pair))
        within_parts.append(jnp.where(low, ahead[0], ahead[1]))
        dscaled_parts.append(jnp.where(low, behind[0], behind[1]))
    within = jnp.concatenate(within_parts, axis=1)
    dscaled = jnp.concatenate(dscaled_parts, axis=1)
    mixed_low = jnp.where(allowed, mixed_grad, 0.0).astype(bf16)
    dc = dc + dot_nn(mixed_low, b_low)
    db = db + dot_tn(mixed_low, c_low)
    fresh_dots = dot_nn(scaled * to_state, tall, highest)
    dcum = dot_nn(dy * (within + from_state) - scaled * dscaled, tall, highest) - fresh_dots
    tail_sum = jnp.sum(fresh_dots, axis=0, keepdims=True) + through_sum
    ddecay = dot_tn(tri, dcum, highest) + tail_sum
    dscaled = dscaled + to_state
    dvalues = step_wide * dscaled + skip_ref[...] * dy
    dstep = dot_nn(dscaled * values, tall, highest) + ddecay * rate_ref[...]
    draw = dstep * sigmoid(raw)
    dskip = jnp.sum(dot_nn(dy * values, tall, highest), axis=0, keepdims=True)
    dhead_ref[0:1, :] += jnp.sum(draw, axis=0, keepdims=True)
    dhead_ref[1:2, :] += jnp.sum(ddecay * decay, axis=0, keepdims=True)
    dhead_ref[2:3, :] += dskip
    dstep_ref[...] = draw.astype(bf16)
    dpre = jnp.concatenate([dvalues, db, dc], axis=1) * slope
    din = weight[3:4, :] * dpre
    dconv_ref[3:4, :] += jnp.sum(dpre * buf[8 : 8 + rows, :], axis=0, keepdims=True)
    dconv_ref[4:5, :] += jnp.sum(dpre, axis=0, keepdims=True)
    dedge = jnp.zeros((8, dpre.shape[1]), f32)
    for tap in range(3):
        masked = dpre * kept[:, tap : tap + 1]
        dconv_ref[tap : tap + 1, :] += jnp.sum(masked * buf[5 + tap : 5 + tap + rows, :], axis=0, keepdims=True)
        grad[0:8, :] = jnp.zeros((8, dpre.shape[1]), f32)
        grad[8 : 8 + rows, :] = masked
        grad[8 + rows :, :] = follow[tap]
        din = din + weight[tap : tap + 1, :] * grad[11 - tap : 11 - tap + rows, :]
        dedge = dedge + weight[tap : tap + 1, :] * grad[3 - tap : 11 - tap, :]
        follow[tap] = masked[0:8, :]
    dedge_ref[...] = dedge
    dx_ref[...] = din[:, :inner].astype(bf16)
    dbc_ref[...] = din[:, inner:].astype(bf16)

    @pl.when(first)
    def _():
        tail_ref[...] = din[rows - 8 :, :]


def attention_kernel(
    low_ref, projected_ref, do_ref, near_ref, far_ref, segc_ref, segr_ref,
    out_ref, dq_ref, dkv_ref, dnear_ref, dfar_ref,
    keys, dkeys, dvalues, q_both, do_both, acc, stats,
    *, scale,
):
    rows = projected_ref.shape[0]
    width = out_ref.shape[1]
    pairs = width // LANES
    blocks = rows // SPAN
    before = segc_ref.shape[0] // rows - 1
    low = lane_low(SPAN)
    high = jnp.logical_not(low)
    zero = jnp.zeros((SPAN, LANES), bf16)
    top_rows = lax.broadcasted_iota(jnp.int32, (LANES, SPAN), 0) < ATT_DIM
    ahead = lax.broadcasted_iota(jnp.int32, (SPAN, SPAN), 1) - lax.broadcasted_iota(jnp.int32, (SPAN, SPAN), 0)
    pick = (
        (lax.broadcasted_iota(jnp.int32, (8, LANES), 1) >= ATT_DIM)
        == (lax.broadcasted_iota(jnp.int32, (8, LANES), 0) == 1)
    ).astype(f32)
    keys[0:rows, :] = far_ref[...]
    keys[rows : 2 * rows, :] = near_ref[...]
    keys[2 * rows :, :] = projected_ref[:, width:]
    dkeys[...] = jnp.zeros_like(dkeys)
    dvalues[...] = jnp.zeros_like(dvalues)

    def halves(value):
        return jnp.where(low, value, zero), jnp.where(high, value, zero)

    def block_step(block, unused):
        q_start = pl.multiple_of(block * SPAN, SPAN)
        q_rows = pl.ds(q_start, SPAN)
        for pair in range(pairs):
            cols = slice(pair * LANES, (pair + 1) * LANES)
            for head, half in enumerate(halves(projected_ref[q_rows, cols] * jnp.asarray(scale, bf16))):
                q_both[2 * pair + head] = half
            for head, half in enumerate(halves(do_ref[q_rows, cols])):
                do_both[2 * pair + head] = half
        segr = segr_ref[:, q_rows]
        first, stop = low_ref[block], before * blocks + block + 1
        acc[...] = jnp.zeros_like(acc)
        stats[0, 0 : 2 * pairs, :] = jnp.full((2 * pairs, SPAN), 0.1 * masked_score, f32)
        stats[1, 0 : 2 * pairs, :] = jnp.zeros((2 * pairs, SPAN), f32)

        def allowed_at(start):
            same = segc_ref[pl.ds(start, SPAN), :] == segr
            return same & (ahead >= start - before * rows - q_start)

        def forward_step(index, unused):
            start = pl.multiple_of(index * SPAN, SPAN)
            allowed = allowed_at(start)
            for pair in range(pairs):
                key = keys[pl.ds(start, SPAN), pair * LANES : (pair + 1) * LANES]
                value = keys[pl.ds(start, SPAN), width + pair * LANES : width + (pair + 1) * LANES]
                value_both = halves(value)
                added = []
                shrink = []
                for head in range(2):
                    one = slice(2 * pair + head, 2 * pair + head + 1)
                    scores = jnp.where(allowed, dot_nt(key, q_both[2 * pair + head]), masked_score)
                    old_top = stats[0, one, :]
                    new_top = jnp.maximum(old_top, jnp.max(scores, axis=0, keepdims=True))
                    weights = jnp.exp(scores - new_top)
                    factor = jnp.exp(old_top - new_top)
                    stats[0, one, :] = new_top
                    stats[1, one, :] = stats[1, one, :] * factor + jnp.sum(weights, axis=0, keepdims=True)
                    shrink.append(factor)
                    added.append(dot_tn(value_both[head], weights.astype(bf16)))
                acc[pair] = acc[pair] * jnp.where(top_rows, shrink[0], shrink[1]) + (added[0] + added[1])
            return unused

        lax.fori_loop(first, stop, forward_step, 0)
        inverse = 1.0 / stats[1, 0 : 2 * pairs, :]
        mass = stats[0, 0 : 2 * pairs, :] + jnp.log(stats[1, 0 : 2 * pairs, :])
        stats[0, 0 : 2 * pairs, :] = mass
        for pair in range(pairs):
            cols = slice(pair * LANES, (pair + 1) * LANES)
            mine = jnp.where(top_rows, inverse[2 * pair : 2 * pair + 1, :], inverse[2 * pair + 1 : 2 * pair + 2, :])
            attended = (acc[pair] * mine).T
            out_ref[q_rows, cols] = attended.astype(bf16)
            delta = dot_nt(pick, do_ref[q_rows, cols].astype(f32) * attended, highest)
            stats[1, 2 * pair : 2 * pair + 2, :] = delta[0:2, :]
        acc[...] = jnp.zeros_like(acc)

        def backward_step(index, unused):
            start = pl.multiple_of(index * SPAN, SPAN)
            where = pl.ds(start, SPAN)
            allowed = allowed_at(start)
            for pair in range(pairs):
                cols = slice(pair * LANES, (pair + 1) * LANES)
                key = keys[where, cols]
                value = keys[where, width + pair * LANES : width + (pair + 1) * LANES]
                key_both = halves(key)
                parts = []
                for head in range(2):
                    one = slice(2 * pair + head, 2 * pair + head + 1)
                    q_one, do_one = q_both[2 * pair + head], do_both[2 * pair + head]
                    scores = jnp.where(allowed, dot_nt(key, q_one), masked_score)
                    weights = jnp.exp(scores - stats[0, one, :])
                    dweights = dot_nt(value, do_one)
                    dscores = (weights * (dweights - stats[1, one, :])).astype(bf16)
                    parts.append(
                        (dot_nn(weights.astype(bf16), do_one), dot_nn(dscores, q_one), dot_tn(key_both[head], dscores))
                    )
                dvalues[where, cols] += parts[0][0] + parts[1][0]
                dkeys[where, cols] += parts[0][1] + parts[1][1]
                acc[pair] += parts[0][2] + parts[1][2]
            return unused

        lax.fori_loop(first, stop, backward_step, 0)
        for pair in range(pairs):
            dq_ref[q_rows, pair * LANES : (pair + 1) * LANES] = (acc[pair] * scale).T
        return unused

    lax.fori_loop(0, blocks, block_step, 0)
    for piece, ref in enumerate((dfar_ref, dnear_ref, dkv_ref)):
        where = slice(piece * rows, (piece + 1) * rows)
        ref[:, :width] = dkeys[where, :].astype(ref.dtype)
        ref[:, width:] = dvalues[where, :].astype(ref.dtype)


def from_behind(value, axis, by):
    count = lax.axis_size(axis)
    pairs = [(i, i + by) for i in range(count) if 0 <= i + by < count]
    return lax.ppermute(value, axis, pairs)


def params(**extra):
    return pltpu.CompilerParams(vmem_limit_bytes=VMEM_LIMIT, **extra)


def cost(flops, moved, transcendentals=0):
    return pl.CostEstimate(flops=int(flops), bytes_accessed=int(moved), transcendentals=int(transcendentals))


def fixed(shape):
    return pl.BlockSpec(shape, lambda *unused: (0,) * len(shape))


def ssd_specs(order, inner, bc_width, state_width):
    per = SPAN // 8
    channels = inner + bc_width

    def before(i):
        return jnp.maximum(order(i) * per - 1, 0)

    return [
        pl.BlockSpec((SPAN, inner), lambda i, *unused: (order(i), 0)),
        pl.BlockSpec((8, inner), lambda i, *unused: (before(i), 0)),
        pl.BlockSpec((SPAN, bc_width + LANES), lambda i, *unused: (order(i), 0)),
        pl.BlockSpec((8, bc_width + LANES), lambda i, *unused: (before(i), 0)),
        fixed((8, channels)),
        pl.BlockSpec((SPAN, 8), lambda i, *unused: (order(i), 0)),
        pl.BlockSpec((SPAN, 1), lambda i, *unused: (order(i), 0)),
        pl.BlockSpec((1, SPAN), lambda i, *unused: (0, order(i))),
    ]


def ssd_constant_specs(inner, channels):
    return [
        fixed((CONV, channels)),
        fixed((1, channels)),
        fixed((1, LANES)),
        fixed((1, LANES)),
        fixed((1, inner)),
        fixed((LANES, inner)),
        fixed((inner, LANES)),
    ]


def ssd_forward(prev, last, zx, bcs, edge, kept, segc, segr, constants, inner, width):
    rows = zx.shape[0]
    blocks = rows // SPAN
    channels = inner + 2 * width
    heads = inner // SSM_DIM
    order = lambda i: i
    return pl.pallas_call(
        ssd_forward_kernel,
        grid_spec=pltpu.PrefetchScalarGridSpec(
            num_scalar_prefetch=2,
            grid=(blocks,),
            in_specs=ssd_specs(order, inner, 2 * width, width) + ssd_constant_specs(inner, channels),
            out_specs=[
                pl.BlockSpec((SPAN, inner), lambda i, *unused: (i, 0)),
                pl.BlockSpec((SPAN, width), lambda i, *unused: (i, 0)),
                pl.BlockSpec((SPAN, LANES), lambda i, *unused: (i, 0)),
                pl.BlockSpec((inner, width), lambda i, *unused: (i, 0)),
                fixed((inner, width)),
                fixed((8, LANES)),
            ],
            scratch_shapes=[
                pltpu.VMEM((inner, width), f32),
                pltpu.VMEM((8, LANES), f32),
                pltpu.VMEM((SPAN + 8, channels), f32),
            ],
        ),
        out_shape=[
            jax.ShapeDtypeStruct((rows, inner), f32),
            jax.ShapeDtypeStruct((rows, width), bf16),
            jax.ShapeDtypeStruct((rows, LANES), f32),
            jax.ShapeDtypeStruct((blocks * inner, width), bf16),
            jax.ShapeDtypeStruct((inner, width), f32),
            jax.ShapeDtypeStruct((8, LANES), f32),
        ],
        compiler_params=params(),
        cost_estimate=cost(rows * SPAN * inner * 6, rows * inner * 12, rows * SPAN * heads),
        name="ssd_forward",
    )(prev, last, zx, zx, bcs, bcs, edge, kept, segc, segr, *constants)


def ssd_backward(prev, last, zx, bcs, edge, kept, segc, segr, dy, states, opened, entering, back_end, constants, inner, width):
    rows = zx.shape[0]
    blocks = rows // SPAN
    channels = inner + 2 * width
    heads = inner // SSM_DIM
    order = lambda i: blocks - 1 - i
    return pl.pallas_call(
        ssd_backward_kernel,
        grid_spec=pltpu.PrefetchScalarGridSpec(
            num_scalar_prefetch=2,
            grid=(blocks,),
            in_specs=ssd_specs(order, inner, 2 * width, width)
            + [
                pl.BlockSpec((SPAN, inner), lambda i, *unused: (order(i), 0)),
                pl.BlockSpec((inner, width), lambda i, *unused: (order(i), 0)),
                pl.BlockSpec((8, LANES), lambda i, *unused: (jnp.maximum(order(i) * (SPAN // 8) - 1, 0), 0)),
                fixed((inner, width)),
                fixed((inner, width)),
            ]
            + ssd_constant_specs(inner, channels),
            out_specs=[
                pl.BlockSpec((SPAN, inner), lambda i, *unused: (order(i), 0)),
                pl.BlockSpec((SPAN, 2 * width), lambda i, *unused: (order(i), 0)),
                pl.BlockSpec((SPAN, LANES), lambda i, *unused: (order(i), 0)),
                fixed((8, channels)),
                fixed((8, channels)),
                fixed((8, channels)),
                fixed((8, LANES)),
            ],
            scratch_shapes=[
                pltpu.VMEM((inner, width), f32),
                pltpu.VMEM((3, 8, channels), f32),
                pltpu.VMEM((SPAN + 8, channels), f32),
                pltpu.VMEM((SPAN + 16, channels), f32),
            ],
        ),
        out_shape=[
            jax.ShapeDtypeStruct((rows, inner), bf16),
            jax.ShapeDtypeStruct((rows, 2 * width), bf16),
            jax.ShapeDtypeStruct((rows, LANES), bf16),
            jax.ShapeDtypeStruct((8, channels), f32),
            jax.ShapeDtypeStruct((8, channels), f32),
            jax.ShapeDtypeStruct((8, channels), f32),
            jax.ShapeDtypeStruct((8, LANES), f32),
        ],
        compiler_params=params(),
        cost_estimate=cost(rows * SPAN * inner * 14, rows * inner * 16, rows * SPAN * heads),
        name="ssd_backward",
    )(prev, last, zx, zx, bcs, bcs, edge, kept, segc, segr, dy, states, opened, entering, back_end, *constants)


def gate_forward(y_zero, state_c, opened, entering, zx, gain, wide):
    rows, inner = y_zero.shape
    width = state_c.shape[1]
    return pl.pallas_call(
        gate_forward_kernel,
        grid=(rows // SPAN,),
        in_specs=[
            pl.BlockSpec((SPAN, inner), lambda i: (i, 0)),
            pl.BlockSpec((SPAN, width), lambda i: (i, 0)),
            pl.BlockSpec((SPAN, LANES), lambda i: (i, 0)),
            fixed((inner, width)),
            pl.BlockSpec((SPAN, inner), lambda i: (i, 0)),
            fixed((1, inner)),
            fixed((LANES, inner)),
        ],
        out_specs=[
            pl.BlockSpec((SPAN, inner), lambda i: (i, 0)),
            pl.BlockSpec((SPAN, inner), lambda i: (i, 0)),
            pl.BlockSpec((8, SPAN), lambda i: (0, i)),
        ],
        out_shape=[
            jax.ShapeDtypeStruct((rows, inner), f32),
            jax.ShapeDtypeStruct((rows, inner), bf16),
            jax.ShapeDtypeStruct((8, rows), f32),
        ],
        compiler_params=params(),
        cost_estimate=cost(rows * inner * width * 4, rows * inner * 14, rows * inner),
        name="gate_forward",
    )(y_zero, state_c, opened, entering, zx, gain, wide)


def gate_backward(back_gated, ssd_out, zx, coefficients, gain, state_c, opened, wide):
    rows, inner = ssd_out.shape
    width = state_c.shape[1]
    return pl.pallas_call(
        gate_backward_kernel,
        grid=(rows // SPAN,),
        in_specs=[
            pl.BlockSpec((SPAN, inner), lambda i: (i, 0)),
            pl.BlockSpec((SPAN, inner), lambda i: (i, 0)),
            pl.BlockSpec((SPAN, inner), lambda i: (i, 0)),
            pl.BlockSpec((SPAN, 8), lambda i: (i, 0)),
            fixed((1, inner)),
            pl.BlockSpec((SPAN, width), lambda i: (i, 0)),
            pl.BlockSpec((SPAN, LANES), lambda i: (i, 0)),
            fixed((LANES, inner)),
        ],
        out_specs=[
            pl.BlockSpec((SPAN, inner), lambda i: (i, 0)),
            pl.BlockSpec((SPAN, inner), lambda i: (i, 0)),
            pl.BlockSpec((SPAN, inner), lambda i: (i, 0)),
            fixed((1, inner)),
            fixed((inner, width)),
        ],
        out_shape=[
            jax.ShapeDtypeStruct((rows, inner), bf16),
            jax.ShapeDtypeStruct((rows, inner), bf16),
            jax.ShapeDtypeStruct((rows, inner), bf16),
            jax.ShapeDtypeStruct((1, inner), f32),
            jax.ShapeDtypeStruct((inner, width), f32),
        ],
        compiler_params=params(),
        cost_estimate=cost(rows * inner * width * 4, rows * inner * 18, rows * inner),
        name="gate_backward",
    )(back_gated, ssd_out, zx, coefficients, gain, state_c, opened, wide)


def attention(low_blocks, projected, back_attended, near, far, segc, segr, att_pad):
    rows = projected.shape[0]
    pairs = att_pad // LANES
    window = segc.shape[0]
    vmem = pl.BlockSpec(memory_space=pltpu.VMEM)
    return pl.pallas_call(
        partial(attention_kernel, scale=1.0 / math.sqrt(ATT_DIM)),
        in_specs=[pl.BlockSpec(memory_space=pltpu.SMEM)] + [vmem] * 6,
        out_specs=[vmem] * 5,
        out_shape=[
            jax.ShapeDtypeStruct((rows, att_pad), bf16),
            jax.ShapeDtypeStruct((rows, att_pad), f32),
            jax.ShapeDtypeStruct((rows, 2 * att_pad), f32),
            jax.ShapeDtypeStruct((rows, 2 * att_pad), bf16),
            jax.ShapeDtypeStruct((rows, 2 * att_pad), bf16),
        ],
        scratch_shapes=[
            pltpu.VMEM((window, 2 * att_pad), bf16),
            pltpu.VMEM((window, att_pad), f32),
            pltpu.VMEM((window, att_pad), f32),
            pltpu.VMEM((2 * pairs, SPAN, LANES), bf16),
            pltpu.VMEM((2 * pairs, SPAN, LANES), bf16),
            pltpu.VMEM((pairs, LANES, SPAN), f32),
            pltpu.VMEM((2, -(-2 * pairs // 8) * 8, SPAN), f32),
        ],
        compiler_params=params(),
        cost_estimate=cost(rows * rows * att_pad * 28, rows * att_pad * 30, rows * rows * pairs * 4),
        name="attention",
    )(low_blocks, projected, back_attended, near, far, segc, segr)


def fit(value, size, axis):
    if value.shape[axis] == size:
        return value
    widths = [(0, 0)] * value.ndim
    widths[axis] = (0, size - value.shape[axis])
    return jnp.pad(value, widths)


def seq_scatter(values):
    return lax.psum_scatter(values.astype(bf16), "seq", scatter_dimension=0, tiled=True).astype(f32)


MESH = pl.DeviceIdType.MESH


class HeadPlace:
    def __init__(self, count):
        self.count = count
        self.chips = count // 2
        self.me = lax.axis_index("head")
        self.core = lax.rem(self.me, 2)
        self.chip = self.me // 2
        self.partner = self.chip * 2 + (1 - self.core)

    def ahead(self, step):
        return lax.rem(self.chip + step, self.chips) * 2 + self.core

    def behind(self, step):
        return lax.rem(self.chip + self.chips - step, self.chips) * 2 + self.core

    def meet(self):
        barrier = pltpu.get_barrier_semaphore()
        others = [self.partner] + [self.ahead(step) for step in range(1, self.chips)]
        for other in others:
            pl.semaphore_signal(barrier, inc=1, device_id={"head": other}, device_id_type=MESH)
        pl.semaphore_wait(barrier, len(others))


def remote(source, target, send, receive, device):
    return pltpu.make_async_remote_copy(
        src_ref=source, dst_ref=target, send_sem=send, recv_sem=receive,
        device_id={"head": device}, device_id_type=MESH,
    )


class TwoLevelGather:
    def __init__(self, place, own_at, full_at, send, receive, parts):
        self.place, self.own_at, self.full_at = place, own_at, full_at
        self.send, self.receive, self.parts = send, receive, parts

    def copy(self, kind, part):
        place = self.place
        slot = kind * self.parts + part
        send, receive = self.send.at[slot], self.receive.at[slot]
        if kind == 0:
            return remote(self.own_at(part), self.full_at(place.me, part), send, receive, place.partner)
        if kind < place.chips:
            return remote(self.own_at(part), self.full_at(place.me, part), send, receive, place.ahead(kind))
        origin = place.behind(kind - place.chips + 1)
        return remote(self.full_at(origin, part), self.full_at(origin, part), send, receive, place.partner)

    def kinds(self):
        return 2 * self.place.chips - 1

    def start(self, part):
        for kind in list(range(1, self.place.chips)) + [0]:
            self.copy(kind, part).start()

    def pass_on(self, part):
        for step in range(1, self.place.chips):
            self.copy(step, part).wait_recv()
            self.copy(self.place.chips + step - 1, part).start()

    def complete(self, part):
        self.copy(0, part).wait_recv()
        for step in range(1, self.place.chips):
            self.copy(self.place.chips + step - 1, part).wait_recv()

    def finish(self, part):
        for kind in range(self.kinds()):
            self.copy(kind, part).wait_send()


class ScalarSum:
    def __init__(self, place, own, near, pair, far, send, receive):
        self.place, self.own, self.near, self.pair, self.far = place, own, near, pair, far
        self.send, self.receive = send, receive

    def first(self):
        return remote(self.own, self.near, self.send.at[0], self.receive.at[0], self.place.partner)

    def second(self, step):
        return remote(
            self.pair, self.far.at[step - 1], self.send.at[step], self.receive.at[step], self.place.ahead(step)
        )

    def start(self):
        self.first().start()

    def middle(self):
        self.first().wait_recv()
        self.pair[...] = self.own[...] + self.near[...]
        for step in range(1, self.place.chips):
            self.second(step).start()

    def total(self):
        total = self.pair[...]
        for step in range(1, self.place.chips):
            self.second(step).wait_recv()
            total = total + self.far[step - 1]
        return total

    def finish(self):
        self.first().wait_send()
        for step in range(1, self.place.chips):
            self.second(step).wait_send()


def column_of(line):
    rows = line.shape[1]
    pick = (lax.broadcasted_iota(jnp.int32, (8, LANES), 0) == 0).astype(f32)
    return dot_tn(jnp.broadcast_to(line, (8, rows)), pick, highest)


def gather_sems(chips, parts):
    slots = (2 * chips - 1) * parts
    return [pltpu.SemaphoreType.DMA((slots,)), pltpu.SemaphoreType.DMA((slots,))]


def scalar_scratch(chips, dense):
    return [
        pltpu.VMEM((dense, LANES), f32),
        pltpu.VMEM((dense, LANES), f32),
        pltpu.VMEM((max(chips - 1, 1), dense, LANES), f32),
        pltpu.SemaphoreType.DMA((chips,)),
        pltpu.SemaphoreType.DMA((chips,)),
    ]


def comm_params(ident):
    return pltpu.CompilerParams(vmem_limit_bytes=VMEM_LIMIT, collective_id=ident, has_side_effects=True)


VMEM = pl.BlockSpec(memory_space=pltpu.VMEM)
CHUNK = 256


def first_gather_kernel(
    count, tokens_ref, gain_ref, zx_ref, bcs_ref, full_ref, rms_ref, z_out, x_out, bcs_out,
    raw, gains, send, receive, gsend, greceive,
):
    rows, features = tokens_ref.shape
    place = HeadPlace(count)
    parts = rows // CHUNK

    def rows_of(part):
        return pl.ds(pl.multiple_of(part * CHUNK, CHUNK), CHUNK)

    data = TwoLevelGather(
        place, lambda part: tokens_ref.at[rows_of(part)], lambda who, part: raw.at[who, rows_of(part)],
        send, receive, parts,
    )
    gain = TwoLevelGather(place, lambda part: gain_ref, lambda who, part: gains.at[who], gsend, greceive, 1)
    place.meet()
    gain.start(0)
    lax.fori_loop(0, parts, lambda part, unused: (data.start(part), unused)[1], 0)
    gains[place.me] = gain_ref[...]
    raw[place.me] = tokens_ref[...]
    gain.pass_on(0)
    gain.complete(0)

    def step(part, unused):
        data.pass_on(part)
        data.complete(part)
        where = rows_of(part)
        values = [raw[who, where, :].astype(f32) for who in range(count)]
        total = sum(jnp.sum(value * value, axis=1, keepdims=True) for value in values)
        scale = lax.rsqrt(total / (count * features) + epsilon)
        rms_ref[where, :] = jnp.broadcast_to(scale, (CHUNK, 8))
        zx = jnp.zeros((CHUNK, zx_ref.shape[1]), f32)
        bcs = jnp.zeros((CHUNK, bcs_ref.shape[1]), f32)
        for who in range(count):
            normed = (values[who] * scale * gains[who, 0:1, :]).astype(bf16)
            full_ref[who, where, :] = normed
            inner_rows = slice(who * features, (who + 1) * features)
            zx = zx + dot_nn(normed, zx_ref[inner_rows, :])
            bcs = bcs + dot_nn(normed, bcs_ref[inner_rows, :])
        inner = z_out.shape[1]
        z_out[where, :] = zx[:, :inner]
        x_out[where, :] = zx[:, inner:]
        bcs_out[where, :] = bcs
        return unused

    lax.fori_loop(0, parts, step, 0)
    gain.finish(0)
    lax.fori_loop(0, parts, lambda part, unused: (data.finish(part), unused)[1], 0)


def first_gather(tokens, gain, zx_weight, bcs_weight, ident):
    rows, features = tokens.shape
    count = D // features
    chips = count // 2
    return pl.pallas_call(
        partial(first_gather_kernel, count),
        in_specs=[VMEM] * 4,
        out_specs=[VMEM] * 5,
        out_shape=[
            jax.ShapeDtypeStruct((count, rows, features), bf16),
            jax.ShapeDtypeStruct((rows, 8), f32),
            jax.ShapeDtypeStruct((rows, zx_weight.shape[1] // 2), f32),
            jax.ShapeDtypeStruct((rows, zx_weight.shape[1] // 2), f32),
            jax.ShapeDtypeStruct((rows, bcs_weight.shape[1]), f32),
        ],
        scratch_shapes=[
            pltpu.VMEM((count, rows, features), bf16),
            pltpu.VMEM((count, 8, features), f32),
        ]
        + gather_sems(chips, rows // CHUNK)
        + gather_sems(chips, 1),
        compiler_params=comm_params(ident),
        cost_estimate=cost(2 * rows * D * (zx_weight.shape[1] + bcs_weight.shape[1]), 30e6),
        name="first_gather",
    )(tokens, fit(gain[None], 8, 0), zx_weight, bcs_weight)


def gather_kernel(count, transposed, scaled, filled, own_ref, dense_ref, weight_ref, *refs):
    fill_left, fill_right = refs[:2] if filled else (None, None)
    refs = refs[2:] if filled else refs
    full_ref, total_ref, out_ref = refs[:3]
    fill_out = refs[3] if filled else None
    send, receive, near, pair, far, ssend, sreceive = refs[-7:]
    rows, features = own_ref.shape
    place = HeadPlace(count)
    parts = rows // CHUNK

    def rows_of(part):
        return pl.ds(pl.multiple_of(part * CHUNK, CHUNK), CHUNK)

    data = TwoLevelGather(
        place, lambda part: own_ref.at[rows_of(part)], lambda who, part: full_ref.at[who, rows_of(part)],
        send, receive, parts,
    )
    scalars = ScalarSum(place, dense_ref, near, pair, far, ssend, sreceive)
    place.meet()
    scalars.start()
    lax.fori_loop(0, parts, lambda part, unused: (data.start(part), unused)[1], 0)
    scalars.middle()
    full_ref[place.me] = own_ref[...]
    total = scalars.total()
    total_ref[...] = total
    if scaled:
        near[...] = lax.rsqrt(total / (count * features) + epsilon)

    def step(part, unused):
        data.pass_on(part)
        if filled:
            for index in range(count // parts):
                who = part * (count // parts) + index
                where = pl.ds(pl.multiple_of(who * features, features), features)
                fill_out[where, :] = dot_tn(fill_left[who], fill_right[...]).astype(bf16)
        data.complete(part)
        where = rows_of(part)
        out = jnp.zeros((CHUNK, out_ref.shape[1]), f32)
        for who in range(count):
            piece = full_ref[who, where, :]
            if transposed:
                out = out + dot_nt(piece, weight_ref[:, who * features : (who + 1) * features])
            else:
                out = out + dot_nn(piece, weight_ref[who * features : (who + 1) * features, :])
        if scaled:
            per = CHUNK // LANES
            line = jnp.concatenate([near[pl.ds(part * per + i, 1), :] for i in range(per)], axis=1)
            out = out * column_of(line)[:, 0:1]
        out_ref[where, :] = out.astype(out_ref.dtype)
        return unused

    lax.fori_loop(0, parts, step, 0)
    scalars.finish()
    lax.fori_loop(0, parts, lambda part, unused: (data.finish(part), unused)[1], 0)


def gather_matmul(own, sums, weight, transposed, scaled, ident, name, fill=()):
    rows, features = own.shape
    count = D // features
    chips = count // 2
    columns = weight.shape[0 if transposed else 1]
    dense = rows // LANES
    shapes = [
        jax.ShapeDtypeStruct((count, rows, features), bf16),
        jax.ShapeDtypeStruct((dense, LANES), f32),
        jax.ShapeDtypeStruct((rows, columns), bf16),
    ]
    if fill:
        shapes.append(jax.ShapeDtypeStruct((D, fill[1].shape[1]), bf16))
    return pl.pallas_call(
        partial(gather_kernel, count, transposed, scaled, bool(fill)),
        in_specs=[VMEM] * (3 + len(fill)),
        out_specs=[VMEM] * len(shapes),
        out_shape=shapes,
        scratch_shapes=gather_sems(chips, rows // CHUNK) + scalar_scratch(chips, dense),
        compiler_params=comm_params(ident),
        cost_estimate=cost(2 * rows * D * columns, 20e6),
        name=name,
    )(own, sums.reshape(dense, LANES), weight, *fill)


def part_rows(part):
    return pl.ds(pl.multiple_of(part * CHUNK, CHUNK), CHUNK)


class TwoLevelScatter:
    def __init__(self, place, lefts, rights, transposed, out, scratch):
        self.place, self.lefts, self.rights, self.transposed, self.out = place, lefts, rights, transposed, out
        (self.own, self.near, self.sent, self.far, self.psend, self.preceive, self.xsend, self.xreceive) = scratch
        self.parts = out.shape[0] // CHUNK

    def to_partner(self, chip, part):
        slot = chip * self.parts + part
        return remote(
            self.own.at[chip * 2 + 1 - self.place.core, part_rows(part)], self.near.at[chip, part_rows(part)],
            self.psend.at[slot], self.preceive.at[slot], self.place.partner,
        )

    def across(self, step, part):
        slot = (step - 1) * self.parts + part
        return remote(
            self.sent.at[step - 1, part_rows(part)], self.far.at[step - 1, part_rows(part)],
            self.xsend.at[slot], self.xreceive.at[slot], self.place.ahead(step),
        )

    def compute(self, part):
        where = part_rows(part)
        features = self.out.shape[1]
        for who in range(self.place.count):
            inner = slice(who * features, (who + 1) * features)
            value = jnp.zeros((CHUNK, features), f32)
            for left, right in zip(self.lefts, self.rights):
                if self.transposed:
                    right, columns = right if isinstance(right, tuple) else (right, slice(None))
                    value = value + dot_nt(left[where, :], right[inner, columns])
                else:
                    value = value + dot_nn(left[where, :], right[:, inner])
            self.own[who, where, :] = value.astype(bf16)
        for chip in range(self.place.chips):
            self.to_partner(chip, part).start()

    def combine(self, part):
        where = part_rows(part)
        place = self.place
        for chip in range(place.chips):
            self.to_partner(chip, part).wait_recv()
        for step in range(1, place.chips):
            chip = lax.rem(place.chip + step, place.chips)
            mine = self.own[chip * 2 + place.core, where, :].astype(f32)
            self.sent[step - 1, where, :] = (mine + self.near[chip, where, :].astype(f32)).astype(bf16)
            self.across(step, part).start()

    def collect(self, part):
        where = part_rows(part)
        place = self.place
        value = self.own[place.me, where, :].astype(f32) + self.near[place.chip, where, :].astype(f32)
        for step in range(1, place.chips):
            self.across(step, part).wait_recv()
            value = value + self.far[step - 1, where, :].astype(f32)
        self.out[where, :] = value

    def drain(self, part):
        for chip in range(self.place.chips):
            self.to_partner(chip, part).wait_send()
        for step in range(1, self.place.chips):
            self.across(step, part).wait_send()


def repeat(start, stop, step):
    lax.fori_loop(start, stop, lambda i, unused: (step(i), unused)[1], 0)


def scatter_scratch(count, rows, features):
    chips = count // 2
    parts = rows // CHUNK
    others = max(chips - 1, 1)
    return [
        pltpu.VMEM((count, rows, features), bf16),
        pltpu.VMEM((chips, rows, features), bf16),
        pltpu.VMEM((others, rows, features), bf16),
        pltpu.VMEM((others, rows, features), bf16),
        pltpu.SemaphoreType.DMA((chips * parts,)),
        pltpu.SemaphoreType.DMA((chips * parts,)),
        pltpu.SemaphoreType.DMA((others * parts,)),
        pltpu.SemaphoreType.DMA((others * parts,)),
    ]


def scatter_kernel(count, operands, transposed, *refs):
    lefts, rights = refs[:operands], refs[operands : 2 * operands]
    dense_ref, out_ref, total_ref = refs[2 * operands : 2 * operands + 3]
    scratch = refs[2 * operands + 3 :]
    place = HeadPlace(count)
    scatter = TwoLevelScatter(place, lefts, rights, transposed, out_ref, scratch[:8])
    scalars = ScalarSum(place, dense_ref, *scratch[8:])
    place.meet()
    scalars.start()
    scatter.compute(0)
    scalars.middle()

    def forward(part):
        scatter.compute(part)
        scatter.combine(part - 1)

    repeat(1, scatter.parts, forward)
    scatter.combine(scatter.parts - 1)
    total_ref[...] = scalars.total()
    repeat(0, scatter.parts, scatter.collect)
    scalars.finish()
    repeat(0, scatter.parts, scatter.drain)


class SeqRing:
    def __init__(self, count):
        self.count = count
        self.me = lax.axis_index("seq")
        self.columns = 2 if count == 8 else 1
        self.place = self.position(self.me)
        self.ahead = self.device(lax.rem(self.place + 1, count))
        self.behind = self.device(lax.rem(self.place + count - 1, count))

    def position(self, index):
        if self.columns == 1:
            return index
        length = self.count // 2
        line, column = index // 2, lax.rem(index, 2)
        return (1 - column) * line + column * (2 * length - 1 - line)

    def device(self, position):
        if self.columns == 1:
            return position
        length = self.count // 2
        column, line = position // length, lax.rem(position, length)
        return 2 * ((1 - column) * line + column * (length - 1 - line)) + column

    def chunk(self, direction, step):
        return self.device(lax.rem(self.place + 2 * self.count - direction * (2 + step), self.count))


def seq_remote(source, target, send, receive, device):
    return pltpu.make_async_remote_copy(
        src_ref=source, dst_ref=target, send_sem=send, recv_sem=receive,
        device_id={"seq": device}, device_id_type=MESH,
    )


class RingStream:
    def __init__(self, ring, direction, source, columns, out, scratch):
        self.ring, self.direction, self.source, self.columns, self.out = ring, direction, source, columns, out
        self.sent, self.got, self.send, self.receive = scratch
        self.rows = source.shape[0] // ring.count

    def copy(self, step):
        device = self.ring.ahead if self.direction == 1 else self.ring.behind
        return seq_remote(
            self.sent.at[step], self.got.at[step], self.send.at[step], self.receive.at[step], device
        )

    def own(self, step):
        chunk = self.ring.chunk(self.direction, step)
        where = pl.ds(pl.multiple_of(chunk * self.rows, self.rows), self.rows)
        return self.source[where, self.columns]

    def start(self):
        self.sent[0] = self.own(-1)
        self.copy(0).start()

    def advance(self, step):
        self.copy(step).wait_recv()
        value = self.got[step].astype(f32) + self.own(step).astype(f32)

        @pl.when(step < self.ring.count - 2)
        def _():
            self.sent[step + 1] = value.astype(bf16)
            self.copy(step + 1).start()

        @pl.when(step == self.ring.count - 2)
        def _():
            self.out[...] = value

    def drain(self, step):
        self.copy(step).wait_send()


def stream_scratch(count, rows, columns):
    return [
        pltpu.VMEM((count - 1, rows, columns), bf16),
        pltpu.VMEM((count - 1, rows, columns), bf16),
        pltpu.SemaphoreType.DMA((count - 1,)),
        pltpu.SemaphoreType.DMA((count - 1,)),
    ]


def tail_kernel(count, streams, state_rows, *refs):
    lefts = refs[:4]
    zx_weight, bc_weight, bcs_weight = refs[4:7]
    refs = refs[7:]
    inner = lefts[0].shape[1]
    bc_width = bc_weight.shape[1]
    rights = (
        (zx_weight, slice(0, inner)),
        (zx_weight, slice(inner, 2 * inner)),
        (bcs_weight, slice(0, bc_width)),
        (bcs_weight, slice(bc_width, bc_width + LANES)),
    )
    dense_ref, small_ref, inner_ref, step_ref, bc_ref, tokens_ref, rms_ref = refs[:7]
    out_ref, total_ref, small_out_ref, bc_out_ref, gain_out_ref = refs[7:12]
    stream_outs = refs[12 : 12 + len(streams) - 1]
    scratch = list(refs[12 + len(streams) - 1 :])

    def take(number):
        taken = scratch[:number]
        del scratch[:number]
        return taken

    place = HeadPlace(count)
    ring = SeqRing(small_out_ref.shape[0])
    scatter = TwoLevelScatter(place, lefts, rights, True, out_ref, take(8))
    scalars = ScalarSum(place, dense_ref, *take(5))
    bc_sum, bc_split, bc_far, bsend, breceive = take(5)
    ssend, sreceive = take(2)
    gains, gsend, greceive = take(3)
    sources = {"inner": inner_ref, "step": step_ref, "bc": bc_ref}
    outs = list(stream_outs) + [bc_sum]
    flows = []
    for (name, direction, columns), out in zip(streams, outs):
        flows.append(RingStream(ring, direction, sources[name], slice(*columns), out, take(4)))

    def small_copy(step):
        block = ring.device(lax.rem(ring.place + ring.count - step, ring.count))
        return seq_remote(
            small_out_ref.at[block], small_out_ref.at[block], ssend.at[step], sreceive.at[step], ring.ahead
        )

    def gain_copy(step):
        return seq_remote(
            gains.at[ring.me], gains.at[ring.me], gsend.at[step - 1], greceive.at[step - 1],
            lax.rem(ring.me + step, ring.count),
        )

    def collected(part):
        scatter.collect(part)
        where = part_rows(part)
        value = tokens_ref[where, :].astype(f32) * rms_ref[where, 0:1] * out_ref[where, :]
        gains[ring.me, 0:1, :] += jnp.sum(value, axis=0, keepdims=True)

    def bc_copy(step):
        other = lax.rem(place.me + step, count)
        return remote(bc_split.at[other], bc_far.at[step - 1], bsend.at[step - 1], breceive.at[step - 1], other)

    barrier = pltpu.get_barrier_semaphore()
    for step in range(1, count):
        pl.semaphore_signal(
            barrier, inc=1, device_id={"head": lax.rem(place.me + step, count)}, device_id_type=MESH
        )
    for step in range(1, ring.count):
        pl.semaphore_signal(
            barrier, inc=1, device_id={"seq": lax.rem(ring.me + step, ring.count)}, device_id_type=MESH
        )
    pl.semaphore_wait(barrier, count - 1 + ring.count - 1)

    scalars.start()
    for flow in flows:
        flow.start()
    scatter.compute(0)
    scalars.middle()
    total = scalars.total()
    total_ref[...] = total
    small_out_ref[ring.me] = small_ref[...]
    small_out_ref[ring.me, 0:state_rows, :] = total[total.shape[0] - state_rows :, :]
    small_copy(0).start()
    gains[ring.me] = jnp.zeros(gains.shape[1:], f32)

    def turn(step):
        for flow in flows:
            flow.advance(step)
        small_copy(step).wait_recv()

        @pl.when(step < ring.count - 2)
        def _():
            small_copy(step + 1).start()

    def forward(part):
        turn(part - 1)
        scatter.compute(part)
        scatter.combine(part - 1)

    repeat(1, scatter.parts, forward)
    scatter.combine(scatter.parts - 1)

    def collect(part):
        turn(scatter.parts - 1 + part)
        collected(part)

    both = min(scatter.parts, ring.count - scatter.parts)
    repeat(0, both, collect)
    repeat(both, scatter.parts, collected)
    repeat(1, ring.count, lambda step: gain_copy(step).start())
    repeat(scatter.parts - 1 + both, ring.count - 1, turn)
    shared = bc_out_ref.shape[0]
    whole = bc_sum[...]
    for who in range(count):
        bc_split[who] = whole[who * shared : (who + 1) * shared, :]
    for step in range(1, count):
        bc_copy(step).start()
    repeat(1, ring.count, lambda step: gain_copy(step).wait_recv())
    gained = gains[0]
    for index in range(1, ring.count):
        gained = gained + gains[index]
    gain_out_ref[...] = gained
    repeat(1, ring.count, lambda step: gain_copy(step).wait_send())
    scalars.finish()
    repeat(0, scatter.parts, scatter.drain)
    for flow in flows:
        repeat(0, ring.count - 1, flow.drain)
    repeat(0, ring.count - 1, lambda step: small_copy(step).wait_send())
    value = bc_split[place.me]
    for step in range(1, count):
        bc_copy(step).wait_recv()
        value = value + bc_far[step - 1]
    bc_out_ref[...] = value
    for step in range(1, count):
        bc_copy(step).wait_send()


def tail(lefts, zx_weight, bc_weight, bcs_weight, sums, state, small, inner_grad, step_grad, bc_grad, tokens, rms, count, ident):
    rows = lefts[0].shape[0]
    features = D // count
    chips = count // 2
    shards = lax.axis_size("seq")
    inner = inner_grad.shape[1]
    width = bc_grad.shape[0]
    total = inner + LANES + width
    first = min(inner, (total + 2 * LANES - 1) // (2 * LANES) * LANES)
    streams = [("inner", 1, (0, first))]
    if first < inner:
        streams.append(("inner", -1, (first, inner)))
    streams.append(("step", -1, (0, LANES)))
    streams.append(("bc", -1, (0, D)))
    per = D // shards
    bc_rows = width // shards
    shared = bc_rows // count
    state_rows = state.shape[0]
    dense = rows // LANES + state_rows
    sizes = [(bc_rows if name == "bc" else per, stop - start) for name, way, (start, stop) in streams]
    flops = sum(2 * rows * D * left.shape[1] for left in lefts)
    block = jnp.concatenate([sums.reshape(rows // LANES, LANES), state], axis=0)
    return pl.pallas_call(
        partial(tail_kernel, count, streams, state_rows),
        in_specs=[VMEM] * 14,
        out_specs=[VMEM] * (5 + len(streams) - 1),
        out_shape=[
            jax.ShapeDtypeStruct((rows, features), f32),
            jax.ShapeDtypeStruct((dense, LANES), f32),
            jax.ShapeDtypeStruct((shards,) + small.shape, f32),
            jax.ShapeDtypeStruct((shared, D), f32),
            jax.ShapeDtypeStruct((8, features), f32),
        ]
        + [jax.ShapeDtypeStruct(size, f32) for size in sizes[:-1]],
        scratch_shapes=scatter_scratch(count, rows, features)
        + scalar_scratch(chips, dense)
        + [
            pltpu.VMEM((bc_rows, D), f32),
            pltpu.VMEM((count, shared, D), f32),
            pltpu.VMEM((count - 1, shared, D), f32),
            pltpu.SemaphoreType.DMA((count - 1,)),
            pltpu.SemaphoreType.DMA((count - 1,)),
            pltpu.SemaphoreType.DMA((shards - 1,)),
            pltpu.SemaphoreType.DMA((shards - 1,)),
            pltpu.VMEM((shards, 8, features), f32),
            pltpu.SemaphoreType.DMA((shards - 1,)),
            pltpu.SemaphoreType.DMA((shards - 1,)),
        ]
        + [item for size in sizes for item in stream_scratch(shards, *size)],
        compiler_params=comm_params(ident),
        cost_estimate=cost(flops, 40e6),
        name="tail",
    )(*lefts, zx_weight, bc_weight, bcs_weight, block, small, inner_grad, step_grad, bc_grad, tokens, rms)


def matmul_scatter(lefts, rights, sums, transposed, count, ident, name):
    rows = lefts[0].shape[0]
    features = D // count
    dense = rows // LANES
    flops = sum(2 * rows * D * left.shape[1] for left in lefts)
    return pl.pallas_call(
        partial(scatter_kernel, count, len(lefts), transposed),
        in_specs=[VMEM] * (2 * len(lefts) + 1),
        out_specs=[VMEM] * 2,
        out_shape=[
            jax.ShapeDtypeStruct((rows, features), f32),
            jax.ShapeDtypeStruct((dense, LANES), f32),
        ],
        scratch_shapes=scatter_scratch(count, rows, features) + scalar_scratch(count // 2, dense),
        compiler_params=comm_params(ident),
        cost_estimate=cost(flops, 20e6),
        name=name,
    )(*lefts, *rights, sums.reshape(dense, LANES))


def weight_grad_kernel(products, left_ref, *refs):
    left = left_ref[...]
    for right, out in zip(refs[:products], refs[products:]):
        out[...] = dot_tn(left, right[...]).astype(out.dtype)


def weight_grad(full, rights, name):
    count, rows, features = full.shape
    columns = [right.shape[1] for right in rights]
    return pl.pallas_call(
        partial(weight_grad_kernel, len(rights)),
        grid=(count,),
        in_specs=[pl.BlockSpec((None, rows, features), lambda i: (i, 0, 0))] + [fixed((rows, n)) for n in columns],
        out_specs=[pl.BlockSpec((features, n), lambda i: (i, 0)) for n in columns],
        out_shape=[jax.ShapeDtypeStruct((count * features, n), bf16) for n in columns],
        compiler_params=params(),
        cost_estimate=cost(2 * rows * D * sum(columns), 2 * (rows + D) * (D + sum(columns))),
        name=name,
    )(full, *rights)


def gathered_product_kernel(full_ref, weight_ref, out_ref):
    count, rows, features = full_ref.shape
    value = jnp.zeros(out_ref.shape, f32)
    for who in range(count):
        value = value + dot_nt(full_ref[who], weight_ref[:, who * features : (who + 1) * features])
    out_ref[...] = value.astype(out_ref.dtype)


def gathered_product(full, weight, name):
    count, rows, features = full.shape
    columns = weight.shape[0]
    return pl.pallas_call(
        gathered_product_kernel,
        grid=(rows // CHUNK,),
        in_specs=[pl.BlockSpec((count, CHUNK, features), lambda i: (0, i, 0)), fixed(weight.shape)],
        out_specs=pl.BlockSpec((CHUNK, columns), lambda i: (i, 0)),
        out_shape=jax.ShapeDtypeStruct((rows, columns), bf16),
        compiler_params=params(),
        cost_estimate=cost(2 * rows * D * columns, 2 * (rows * D + D * columns + rows * columns)),
        name=name,
    )(full, weight)


def spread_product_kernel(left_ref, weight_ref, out_ref):
    features = out_ref.shape[2]
    for who in range(out_ref.shape[0]):
        out_ref[who] = dot_nn(left_ref[...], weight_ref[:, who * features : (who + 1) * features]).astype(out_ref.dtype)


def spread_product(left, weight, count, name):
    rows, depth = left.shape
    features = weight.shape[1] // count
    return pl.pallas_call(
        spread_product_kernel,
        grid=(rows // CHUNK,),
        in_specs=[pl.BlockSpec((CHUNK, depth), lambda i: (i, 0)), fixed(weight.shape)],
        out_specs=pl.BlockSpec((count, CHUNK, features), lambda i: (0, i, 0)),
        out_shape=jax.ShapeDtypeStruct((count, rows, features), bf16),
        compiler_params=params(),
        cost_estimate=cost(2 * rows * D * depth, 2 * (rows * D + D * depth + rows * depth)),
        name=name,
    )(left, weight)


def per_device(
    tokens, segment_ids, first_gain, proj_zx, proj_bc, proj_step, conv_inner, conv_inner_bias,
    conv_state, conv_state_bias, step_bias, decay_log, skip_scale, gated_gain, proj_out,
    second_gain, proj_qkv, attention_out, cotangent,
):
    rows = tokens.shape[0]
    inner = proj_zx.shape[2]
    bc_width = proj_bc.shape[1]
    width = bc_width // 2
    channels = inner + bc_width
    heads = step_bias.shape[0]
    att = proj_qkv.shape[2]
    att_pad = -(-att // LANES) * LANES
    pairs = att_pad // LANES
    blocks = rows // SPAN
    reach = (DOC_MAX - 2) // rows + 1
    row_start = lax.axis_index("seq") * rows

    padded_seg = jnp.concatenate([jnp.full((reach * rows,), -1, jnp.int32), segment_ids])
    window = lax.dynamic_slice_in_dim(padded_seg, row_start, (reach + 1) * rows)
    local_seg = window[reach * rows :]
    shifted = window[reach * rows - (CONV - 1) :]
    kept = jnp.stack([(shifted[tap : tap + rows] == local_seg).astype(f32) for tap in range(CONV - 1)], axis=1)
    kept = fit(kept, 8, 1)
    span_prev = shifted[CONV - 2 :: SPAN][:blocks]
    span_last = local_seg[SPAN - 1 :: SPAN]
    segc_window = window[:, None]
    segc = local_seg[:, None]
    segr = local_seg[None, :]
    key_last = window[SPAN - 1 :: SPAN]
    low_blocks = jnp.sum((key_last[None, :] < local_seg[::SPAN][:, None]).astype(jnp.int32), axis=1)

    owner = jnp.arange(inner, dtype=jnp.int32)[None, :] // SSM_DIM
    wide = (owner == jnp.arange(LANES, dtype=jnp.int32)[:, None]).astype(f32)
    tall = wide.T
    constants = (
        jnp.concatenate([conv_inner, conv_state], axis=1),
        jnp.concatenate([conv_inner_bias, conv_state_bias])[None],
        fit(step_bias[None], LANES, 1),
        fit(-jnp.exp(decay_log)[None], LANES, 1),
        jnp.repeat(skip_scale, SSM_DIM)[None],
        wide,
        tall,
    )
    count = lax.axis_size("head")
    zx_weight = proj_zx.reshape(D, 2 * inner)
    bcs_weight = jnp.concatenate([proj_bc, fit(proj_step, LANES, 1)], axis=1)
    qkv_weight = fit(proj_qkv, att_pad, 2).reshape(D, 3 * att_pad)
    att_weight = fit(attention_out, att_pad, 0)

    first_full, first_rms, zed, inner_x, bcs = first_gather(
        tokens, first_gain, zx_weight, bcs_weight, 0
    )
    rms_columns = first_rms
    first_rms = first_rms[:, 0:1]
    cot_full = lax.all_gather(cotangent, "head")
    edge_rows = jnp.concatenate([inner_x[rows - 8 :], bcs[rows - 8 :, :bc_width]], axis=1)
    edge = from_behind(edge_rows, "seq", 1)

    ssd_shared = (span_prev, span_last, inner_x, bcs, edge, kept, segc, segr)
    y_zero, state_c, opened, states, end_state, through = ssd_forward(*ssd_shared, constants, inner, width)

    sent = end_state.astype(bf16)
    packed = jnp.concatenate([sent, jnp.broadcast_to(through[0:1], (8, LANES)).astype(bf16)], axis=0)
    near_pack = from_behind(packed, "seq", 1).astype(f32)
    near_through = jnp.repeat(near_pack[inner, :heads], SSM_DIM)[:, None]
    far = from_behind(sent, "seq", 2).astype(f32)
    entering = (near_pack[:inner] + near_through * far).astype(bf16)

    ssd_out, gated_raw, gate_sums = gate_forward(y_zero, state_c, opened, entering, zed, gated_gain[None], wide)
    branch_raw, gate_total = matmul_scatter(
        (gated_raw,), (proj_out,), gate_sums[0], False, count, 1, "branch_scatter"
    )
    gate_rms = lax.rsqrt(gate_total.reshape(rows, 1) / INNER + epsilon)
    branch = branch_raw * gate_rms
    hidden_zero = tokens.astype(f32)
    hidden_one = hidden_zero + branch
    second_full, second_total, projected = gather_matmul(
        (hidden_one * second_gain).astype(bf16), jnp.sum(hidden_one * hidden_one, axis=1),
        qkv_weight, False, True, 2, "second_gather",
    )
    second_rms = lax.rsqrt(second_total.reshape(rows, 1) / D + epsilon)
    key_value = projected[:, att_pad:]
    moved = [from_behind(key_value, "seq", back) for back in range(1, reach + 1)]

    back_attended = gathered_product(cot_full, att_weight, "back_attended")
    near_pair, far_pair = moved
    attended, back_query, back_pair, *back_moved = attention(
        low_blocks, projected, back_attended, near_pair, far_pair, segc_window, segr, att_pad
    )
    out_part = spread_product(attended, att_weight, count, "output_product")
    (grad_att,) = weight_grad(cot_full, (attended,), "grad_attention_out")

    returned = [from_behind(back_moved[back - 1], "seq", -back) for back in range(1, reach + 1)]
    *returned, out_part, grad_att = lax.optimization_barrier((*returned, out_part, grad_att))
    back_pair = back_pair + sum(pair.astype(f32) for pair in returned)
    back_projected = jnp.concatenate([back_query, back_pair], axis=1).astype(bf16)
    output = (
        hidden_one + lax.psum_scatter(out_part, "head", scatter_dimension=0).astype(f32)
    ).astype(bf16)
    second_sums = jnp.sum(back_projected.astype(f32) * projected.astype(f32), axis=1)
    back_second, second_dots = matmul_scatter(
        (back_projected,), (qkv_weight,), second_sums, True, count, 3, "second_scatter"
    )
    grad_second_gain = jnp.sum(hidden_one * second_rms * back_second, axis=0)
    back_hidden_one = (
        cotangent.astype(f32)
        + second_rms * second_gain * back_second
        - hidden_one * (second_rms * second_rms / D * second_dots.reshape(rows, 1))
    )
    back_low = back_hidden_one.astype(bf16)
    back_branch, gate_dots, back_gated, grad_qkv = gather_matmul(
        back_low, jnp.sum(back_low.astype(f32) * branch, axis=1), proj_out, True, False, 4, "branch_gather",
        (second_full, (back_projected.astype(f32) * second_rms).astype(bf16)),
    )
    if att != att_pad:
        grad_att = grad_att[:, :att]
        grad_qkv = grad_qkv.reshape(D, 3, att_pad)[:, :, :att].reshape(D, 3 * att)
    coefficients = fit(
        jnp.concatenate([gate_rms, gate_rms * gate_rms / INNER * gate_dots.reshape(rows, 1)], axis=1), 8, 1
    )
    dy, back_z, gated, grad_gated_gain, back_entering = gate_backward(
        back_gated, ssd_out, zed, coefficients, gated_gain[None], state_c, opened, wide
    )

    back_sent = back_entering.astype(bf16)
    back_pack = jnp.concatenate([back_sent, jnp.broadcast_to(through[0:1], (8, LANES)).astype(bf16)], axis=0)
    back_near_pack = from_behind(back_pack, "seq", -1).astype(f32)
    back_far = from_behind(back_sent, "seq", -2).astype(f32)
    back_near_through = jnp.repeat(back_near_pack[inner, :heads], SSM_DIM)[:, None]
    back_end = back_near_pack[:inner] + back_near_through * back_far
    (grad_out,) = weight_grad(back_branch, (gated,), "grad_out")
    (grad_gate,) = weight_grad(first_full, (back_z,), "grad_gate")

    back_end, grad_out, grad_gate = lax.optimization_barrier((back_end, grad_out, grad_gate))
    back_x, back_bc, back_step, tail_rows, back_edge, grad_conv, grad_heads = ssd_backward(
        *ssd_shared, dy, states, opened, entering, back_end, constants, inner, width
    )
    tail_rows = (tail_rows + from_behind(back_edge, "seq", -1)).astype(bf16)
    back_x = lax.dynamic_update_slice(back_x, tail_rows[:, :inner], (rows - 8, 0))
    back_bc = lax.dynamic_update_slice(back_bc, tail_rows[:, inner:], (rows - 8, 0))
    grad_inner, grad_bc, grad_step = weight_grad(first_full, (back_x, back_bc, back_step), "grad_inner")
    first_sums = (
        jnp.sum(back_z.astype(f32) * zed, axis=1)
        + jnp.sum(back_x.astype(f32) * inner_x, axis=1)
        + jnp.sum(back_bc.astype(f32) * bcs[:, :bc_width], axis=1)
        + jnp.sum(back_step.astype(f32) * bcs[:, bc_width:], axis=1)
    )
    small_parts = (grad_conv[:5, :inner], grad_gated_gain[0], grad_second_gain, grad_heads[:3].reshape(-1))
    flat = jnp.concatenate([part.reshape(-1) for part in small_parts])
    state_rows = 16
    state = fit(grad_conv[:5, inner:].reshape(-1, LANES), state_rows, 0)
    lines = -(-flat.size // (8 * LANES)) * 8
    small = jnp.concatenate([jnp.zeros((state_rows, LANES), f32), fit(flat, lines * LANES, 0).reshape(lines, LANES)], axis=0)
    back_first, totals, small_all, shared_bc, first_sum, *wide_tail, wide_step = tail(
        (back_z, back_x, back_bc, back_step), zx_weight, proj_bc, bcs_weight,
        first_sums, state, small, grad_inner, grad_step, grad_bc.T, tokens, rms_columns, count, 5,
    )
    first_dots = totals[: rows // LANES]
    grad_tokens = (
        back_hidden_one
        + first_rms * first_gain * back_first
        - hidden_zero * (first_rms * first_rms / D * first_dots.reshape(rows, 1))
    ).astype(bf16)

    wide_att = seq_scatter(grad_att).T
    wide_qkv = seq_scatter(grad_qkv).reshape(-1, 3, att)
    wide_out = seq_scatter(grad_out).T
    wide_gate = seq_scatter(grad_gate)
    wide_zx = jnp.stack([wide_gate, jnp.concatenate(wide_tail, axis=1)], axis=1)
    wide_step = wide_step[:, :heads]
    small = jnp.sum(small_all, axis=0)
    state_sum = small[:10].reshape(5, bc_width)
    flat = small[state_rows:].reshape(-1)
    picked = []
    at = 0
    for part in small_parts:
        picked.append(flat[at : at + part.size].reshape(part.shape))
        at += part.size
    conv_sum, gated_sum, second_sum, heads_sum = picked
    heads_sum = heads_sum.reshape(3, LANES)[:, :heads]
    shared = bc_width // (lax.axis_size("seq") * count)
    shared_at = (lax.axis_index("seq") * count + lax.axis_index("head")) * shared
    shared_conv = lax.dynamic_slice_in_dim(state_sum, shared_at, shared, 1)
    return (
        output,
        grad_tokens,
        first_sum[0],
        wide_zx,
        shared_bc.T,
        wide_step,
        conv_sum[:4],
        conv_sum[4],
        shared_conv[:4],
        shared_conv[4],
        heads_sum[0],
        heads_sum[1],
        heads_sum[2],
        gated_sum,
        wide_out,
        second_sum,
        wide_qkv,
        wide_att,
    )


def solution(mesh):
    placed = (
        P("seq", "head"),
        P(),
        P("head"),
        P(None, None, "head"),
        P(),
        P(None, "head"),
        P(None, "head"),
        P("head"),
        P(),
        P(),
        P("head"),
        P("head"),
        P("head"),
        P("head"),
        P("head", None),
        P("head"),
        P(None, None, "head"),
        P("head", None),
        P("seq", "head"),
    )
    return jax.shard_map(
        per_device,
        mesh=mesh,
        in_specs=placed,
        out_specs=(
            P("seq", "head"),
            P("seq", "head"),
            P("head"),
            P("seq", None, "head"),
            P(None, ("seq", "head")),
            P("seq", "head"),
            P(None, "head"),
            P("head"),
            P(None, ("seq", "head")),
            P(("seq", "head")),
            P("head"),
            P("head"),
            P("head"),
            P("head"),
            P("head", "seq"),
            P("head"),
            P("seq", None, "head"),
            P("head", "seq"),
        ),
        check_vma=False,
    )
```
